32 devices in a mesh: inner: 4 (over z), outer: 8 (over y, x, core).
Axes of the slice: x: 2, y: 2, z: 4, core: 2. Of those that a mesh axis runs over, the one named last changes fastest.
Arguments:
- inner_state: float32 [2, 16, 2048], P(None, 'inner', 'outer'), may hold values from -6 to 6
- outer_state: float32 [2, 640, 4096], P(None, 'inner', 'outer'), may hold values from -6 to 6
- energies: float32 [16, 2048], P('inner', 'outer'), may hold values from -2 to 2
- dipole: float32 [16, 2048, 2048], P('inner', 'outer'), may hold values from -0.125 to 0.125
- surface: float32 [16, 40, 2048], P('inner', None, 'outer'), may hold values from -0.125 to 0.125
- thresholds: float32 [640], P('inner'), may hold values from 0 to 2
- coupling_coef: float32 [16, 40, 40], P('inner'), may hold values from -1 to 1
- coupling_pattern: int32 [16, 40, 40], P('inner'), may hold values 0 or 1
- block_sizes: int32 [16], P('inner'), may hold values from 1 to 2048, 30720 in all
- field_strength: float32 [2], replicated, may hold values from 0.5 to 2
Outputs:
- inner_final: float32 [2, 16, 2048], P(None, 'inner', 'outer')
- outer_final: float32 [2, 640, 4096], P(None, 'inner', 'outer')
The draws below stay inside these ranges and needn't reach their ends.
All inputs are finite; a program needn't handle non-finite values. No bound on the sum of `coupling_pattern` or of `block_sizes` on one device may be relied on, other than what follows from the above.
Results may differ from the reference program's by a relative error of at most 0.0001.
Values sent between devices are 32-bit elements; how exact they have to be, the bound alone decides.
A program may use at most 128 MiB of HBM per device.

```python
import math
import jax
import jax.numpy as jnp
import numpy as np
from jax import lax

BMAX = 2048
CHL = 40
STEPS = 2
ORDER = 4
NL = 16
NC = 640
NR = 4096


def touch_ends(entries, key, low, high):
    longest = entries.shape.index(max(entries.shape))
    spots = []
    for shift in (0, 1):
        where = [jax.random.randint(jax.random.fold_in(key, axis), (), 0, length) for axis, length in enumerate(entries.shape)]
        where[longest] = (where[longest] + shift) % entries.shape[longest]
        spots.append(tuple(where))
    return entries.at[spots[0]].set(low).at[spots[1]].set(high)


def shard_levels(rng, extent, split, least, largest):
    factor_of, own = 1.0, jax.random.fold_in(rng, 6)
    for position, parts in split:
        draws = jnp.exp(jax.random.uniform(jax.random.fold_in(own, position), (parts,), jnp.float32, least / len(split), largest / len(split)))
        factor_of = factor_of * jnp.repeat(draws, extent[position] // parts).reshape([-1 if axis == position else 1 for axis in range(len(extent))])
    return factor_of


def length_profile(amount, total, reach, lean):
    loads = [(1 << 20) // math.isqrt(rank ** lean) + 1 for rank in range(2, amount + 1)]
    surplus, given = total - reach - (amount - 1), [1] * (amount - 1)
    while surplus > 0:
        free = [i for i in range(amount - 1) if given[i] < reach]
        whole, left = sum([loads[i] for i in free]), surplus
        for i in free:
            addition = min(reach - given[i], max(1, left * loads[i] // whole), surplus)
            given[i] = given[i] + addition
            surplus = surplus - addition
    return np.array([reach] + given)


def ragged(stream_key, amount, total, reach, slope):
    if amount == 2:
        one = jax.random.randint(stream_key, (), max(1, total - reach), min(reach, total - 1) + 1)
        return jnp.stack([one, total - one])
    sizes = jnp.asarray(length_profile(amount, total, reach, slope), jnp.int32)
    pairs = (amount - 1) // 2
    giver, taker = sizes[1:1 + 2 * pairs:2], sizes[2:2 + 2 * pairs:2]
    room = jnp.minimum(giver - 1, reach - taker)
    shifted = jax.random.randint(jax.random.fold_in(stream_key, 1), (pairs,), 0, 1 << 20) % (room + 1)
    sizes = sizes.at[1:1 + 2 * pairs:2].set(giver - shifted).at[2:2 + 2 * pairs:2].set(taker + shifted)
    return sizes[jax.random.permutation(jax.random.fold_in(stream_key, 2), amount)]


def bell_draw(stream_key, shape, width, limit, split=(), held_as=jnp.bfloat16):
    result = width * jax.random.normal(stream_key, shape, jnp.float32)
    if split:
        result = result * shard_levels(stream_key, shape, split, -0.22, 0.18)
    return jnp.clip(result, -limit, limit).astype(held_as)


def setup_inputs(seed: int = 0) -> dict:
    streams_of = jax.random.split(jax.random.key(seed), 11)
    inner_state = bell_draw(streams_of[0], (2, NL, BMAX), 1.0, 6.0, ((1, 4), (2, 8)), jnp.float32)
    outer_state = bell_draw(streams_of[1], (2, NC, NR), 1.0, 6.0, ((1, 4), (2, 8)), jnp.float32)
    energies = jnp.clip(jax.random.uniform(streams_of[2], (NL, BMAX), jnp.float32, -2.0, 2.0) * shard_levels(streams_of[2], (NL, BMAX), ((0, 4), (1, 8)), -0.4, 0.0), -2.0, 2.0)
    dipole = bell_draw(streams_of[3], (NL, BMAX, BMAX), BMAX ** -0.5, 0.125, ((0, 4), (1, 8)), jnp.float32)
    surface = bell_draw(streams_of[4], (NL, CHL, BMAX), BMAX ** -0.5, 0.125, ((0, 4), (2, 8)), jnp.float32)
    thresholds = jnp.clip(2.0 * jax.random.uniform(streams_of[5], (NC,), jnp.float32) ** shard_levels(streams_of[5], (NC,), ((0, 4),), -0.2, 0.2), 0.0, 2.0)
    coupling_coef = bell_draw(streams_of[6], (NL, CHL, CHL), CHL ** -0.5, 1.0, ((0, 4),), jnp.float32)
    coupling_pattern = touch_ends((jax.random.randint(streams_of[7], (NL, CHL, CHL), 0, 2) < 1).astype(jnp.int32), jax.random.fold_in(streams_of[7], 1), 0, 1)
    block_sizes = ragged(streams_of[8], NL, NL * BMAX * 15 // 16, BMAX, 2).astype(jnp.int32)
    field_strength = jnp.clip(jax.random.uniform(streams_of[9], (STEPS,), jnp.float32, 0.5, 2.0), 0.5, 2.0)
    return dict(inner_state=inner_state, outer_state=outer_state, energies=energies, dipole=dipole, surface=surface, thresholds=thresholds, coupling_coef=coupling_coef, coupling_pattern=coupling_pattern, block_sizes=block_sizes, field_strength=field_strength)


kinetic_scale = 3.125
time_step = 0.1


def apply_operator(inner_part, outer_part, live_rows, energies, dipole, surface, thresholds, coupling, strength):
    highest = lax.Precision.HIGHEST
    forward = jnp.einsum('lij,plj->pli', dipole[:-1], inner_part[:, 1:], precision=highest)
    backward = jnp.einsum('lji,plj->pli', dipole[:-1], inner_part[:, :-1], precision=highest)
    zero_block = jnp.zeros((2, 1, BMAX), jnp.float32)
    forward = jnp.concatenate([forward, zero_block], axis=1)
    backward = jnp.concatenate([zero_block, backward], axis=1)
    first_point = outer_part[:, :, 0].reshape(2, NL, CHL)
    surf_term = jnp.einsum('lcs,plc->pls', surface, first_point, precision=highest)
    inner_image = live_rows * (energies * inner_part + strength * (forward + backward) - kinetic_scale * surf_term)
    boundary = jnp.einsum('lcs,pls->plc', surface, inner_part, precision=highest).reshape(2, NC)
    zero_col = jnp.zeros((2, NC, 1), jnp.float32)
    left_cells = jnp.concatenate([boundary[:, :, None], outer_part[:, :, :-1]], axis=2)
    right_cells = jnp.concatenate([outer_part[:, :, 1:], zero_col], axis=2)
    kinetic = kinetic_scale * (2.0 * outer_part - left_cells - right_cells)
    channel_grid = outer_part.reshape(2, NL, CHL, NR)
    upward = jnp.einsum('lab,plbr->plar', coupling[:-1], channel_grid[:, 1:], precision=highest)
    downward = jnp.einsum('lba,plbr->plar', coupling[:-1], channel_grid[:, :-1], precision=highest)
    zero_grid = jnp.zeros((2, 1, CHL, NR), jnp.float32)
    upward = jnp.concatenate([upward, zero_grid], axis=1)
    downward = jnp.concatenate([zero_grid, downward], axis=1)
    outer_image = kinetic + thresholds[None, :, None] * outer_part + strength * (upward + downward).reshape(2, NC, NR)
    return inner_image, outer_image


def reference(inner_state, outer_state, energies, dipole, surface, thresholds, coupling_coef, coupling_pattern, block_sizes, field_strength):
    positions = jnp.arange(BMAX, dtype=jnp.int32)
    live_rows = (positions[None, :] < block_sizes[:, None]).astype(jnp.float32)
    coupling = coupling_coef * coupling_pattern.astype(jnp.float32)
    current = (inner_state * live_rows, outer_state)
    for time_index in range(STEPS):
        strength = field_strength[time_index]
        taylor_term = current
        accumulated = current
        for power in range(1, ORDER + 1):
            inner_image, outer_image = apply_operator(taylor_term[0], taylor_term[1], live_rows, energies, dipole, surface, thresholds, coupling, strength)
            factor = time_step / power
            taylor_term = (factor * jnp.stack([inner_image[1], -inner_image[0]]), factor * jnp.stack([outer_image[1], -outer_image[0]]))
            accumulated = (accumulated[0] + taylor_term[0], accumulated[1] + taylor_term[1])
        current = accumulated
    return current[0], current[1]
```

```python
import functools

import jax
import jax.numpy as jnp
from jax import lax
from jax.experimental import pallas as pl
from jax.experimental.pallas import tpu as pltpu
from jax.sharding import PartitionSpec as P

STEPS = 2
ORDER = 4

kinetic_scale = 3.125
time_step = 0.1

MESH = pl.DeviceIdType.MESH
f32 = jnp.float32
bf16 = jnp.bfloat16
NN = (((1,), (0,)), ((), ()))
SLOTS = 4


def halves(x):
    high = x.astype(bf16).astype(f32)
    return high, x - high


def split(x):
    high = x.astype(bf16)
    return high, (x - high.astype(f32)).astype(bf16)


def dot(a, b):
    return lax.dot_general(a, b, NN, preferred_element_type=f32)


def kernel(
    planes,
    sectors,
    ch,
    inner_ref,
    outer_hbm,
    energy_ref,
    dipole_hbm,
    surface_ref,
    threshold_ref,
    coef_ref,
    pattern_ref,
    size_ref,
    field_ref,
    inner_out,
    outer_out,
    dip_full,
    dip_cat,
    dip_turn,
    surf_cat,
    surf_turn,
    mix_split,
    grid,
    halo_out,
    term,
    peer_in,
    first_out,
    above_in,
    part_out,
    part_in,
    far_out,
    below_in,
    pairs,
    live_ref,
    energy_rows,
    total_inner,
    diag_ref,
    edge_out,
    left_in,
    right_in,
    surf_in,
    point_in,
    sem_load,
    sem_outer,
    sem_g_send,
    sem_g_recv,
    sem_a_send,
    sem_a_recv,
    sem_z_send,
    sem_z_recv,
    sem_b_send,
    sem_b_recv,
    sem_y_send,
    sem_y_recv,
    sem_up_send,
    sem_up_recv,
    sem_down_send,
    sem_down_recv,
    sem_e_send,
    sem_left,
    sem_right,
    sem_surf_send,
    sem_surf,
    sem_point_send,
    sem_point,
):
    z = lax.axis_index("inner")
    me = lax.axis_index("outer")
    blocks, rc = energy_ref.shape
    rows = 2 * blocks
    nc, nr = grid.shape[2] - 2 * ch, grid.shape[3]
    ext = edge_out.shape[2]
    depth = 2 * blocks * rc
    near = rows - 2
    has_below = z > 0
    has_above = z < planes - 1
    power = sectors & (sectors - 1) == 0

    def partner(s):
        if not power:
            return lax.rem(me + s, sectors)
        to, bit = me, 1
        while bit < sectors:
            if s & bit:
                to = to + bit * (1 - 2 * ((me // bit) % 2))
            bit *= 2
        return to

    def source(s):
        return partner(s) if power else lax.rem(me + sectors - s, sectors)

    def remote(src, dst, send, recv, plane, sector):
        return pltpu.make_async_remote_copy(
            src_ref=src,
            dst_ref=dst,
            send_sem=send,
            recv_sem=recv,
            device_id={"inner": plane, "outer": sector},
            device_id_type=MESH,
        )

    def wait(ref, sem):
        pltpu.make_async_copy(ref, ref, sem).wait()

    barrier = pltpu.get_barrier_semaphore()

    def greet(plane, s):
        pl.semaphore_signal(
            barrier,
            inc=1,
            device_id={"inner": plane, "outer": partner(s)},
            device_id_type=MESH,
        )

    for s in range(sectors - 1, 0, -1):
        greet(z, s)

    @pl.when(has_below)
    def _():
        for s in range(sectors - 1, -1, -1):
            greet(z - 1, s)

    @pl.when(has_above)
    def _():
        for s in range(sectors - 1, -1, -1):
            greet(z + 1, s)

    own = pl.ds(ch, nc)
    states = []
    for p in range(2):
        states.append(
            pltpu.make_async_copy(outer_hbm.at[p], grid.at[0, p, own, :], sem_outer.at[p])
        )
        states.append(
            pltpu.make_async_copy(
                outer_hbm.at[p, pl.ds(nc - ch, ch)], halo_out.at[p, 0], sem_outer.at[2 + p]
            )
        )
        states.append(
            pltpu.make_async_copy(
                outer_hbm.at[p, pl.ds(0, ch)], halo_out.at[p, 1], sem_outer.at[4 + p]
            )
        )
        states.append(
            pltpu.make_async_copy(outer_hbm.at[p], outer_out.at[p], sem_outer.at[6 + p])
        )
    for state in states:
        state.start()
    loads = [
        pltpu.make_async_copy(
            dipole_hbm.at[pl.ds(l * rc, rc)], dip_full.at[pl.ds(l * rc, rc)], sem_load.at[l]
        )
        for l in range(blocks)
    ]
    for load in loads:
        load.start()

    @pl.when(z == 0)
    def _():
        below_in[...] = jnp.zeros_like(below_in)
        grid[:, :, 0:ch, :] = jnp.zeros((2, 2, ch, nr), f32)

    @pl.when(z == planes - 1)
    def _():
        above_in[...] = jnp.zeros_like(above_in)
        grid[:, :, ch + nc : 2 * ch + nc, :] = jnp.zeros((2, 2, ch, nr), f32)

    def channel_copies(slot, p):
        up = remote(
            halo_out.at[p, 0],
            grid.at[slot, p, pl.ds(0, ch), :],
            sem_up_send.at[p],
            sem_up_recv.at[slot, p],
            z + 1,
            me,
        )
        down = remote(
            halo_out.at[p, 1],
            grid.at[slot, p, pl.ds(ch + nc, ch), :],
            sem_down_send.at[p],
            sem_down_recv.at[slot, p],
            z - 1,
            me,
        )
        return up, down

    side = pairs.shape[1]
    for l in range(blocks + 1):
        pairs[l, ch:side, :] = jnp.zeros((side - ch, side), f32)
    for l in range(blocks):
        pairs[l + 1, 0:ch, :] = jnp.zeros((ch, side), f32)
        pairs[l + 1, 0:ch, 0:ch] = coef_ref[l] * pattern_ref[l].astype(f32)

    @pl.when(z == 0)
    def _():
        pairs[0, 0:ch, :] = jnp.zeros((ch, side), f32)

    share = remote(
        pairs.at[blocks, pl.ds(0, ch), :],
        pairs.at[0, pl.ds(0, ch), :],
        sem_g_send,
        sem_g_recv,
        z + 1,
        me,
    )

    order_of = [(l, p) for l in range(blocks) for p in range(2)]
    position = me * rc + lax.broadcasted_iota(jnp.int32, (1, rc), 1)
    live_ref[...] = jnp.concatenate(
        [jnp.where(position < size_ref[l], 1.0, 0.0) for l, p in order_of], axis=0
    )
    energy_rows[...] = jnp.concatenate([energy_ref[l : l + 1, :] for l, p in order_of], axis=0)
    term[...] = live_ref[...] * jnp.concatenate(
        [inner_ref[p, l : l + 1, :] for l, p in order_of], axis=0
    )
    total_inner[...] = term[...]

    small = lax.broadcasted_iota(jnp.int32, (nc, nc), 0) == lax.broadcasted_iota(
        jnp.int32, (nc, nc), 1
    )
    diag_ref[...] = 2.0 * kinetic_scale + jnp.sum(
        jnp.where(small, threshold_ref[...], 0.0), axis=1, keepdims=True
    )

    surface_ext = jnp.concatenate(
        [
            jnp.zeros((ch, rc), f32),
            surface_ref[...],
            jnp.zeros((ext - ch - nc, rc), f32),
        ],
        axis=0,
    )
    sh, sl = split(surface_ext)
    surf_cat[0:ext, :] = sh
    surf_cat[ext : 2 * ext, :] = sl
    surf_turn[0:rc, :] = sh.T
    surf_turn[rc : 2 * rc, :] = sl.T

    waits = (sectors - 1) + sectors * (
        jnp.where(has_below, 1, 0) + jnp.where(has_above, 1, 0)
    )
    pl.semaphore_wait(barrier, waits)

    @pl.when(has_above)
    def _():
        share.start()

    for p in (1, 0):
        states[4 * p + 1].wait()
        states[4 * p + 2].wait()
        up, down = channel_copies(0, p)

        @pl.when(has_above)
        def _():
            up.start()

        @pl.when(has_below)
        def _():
            down.start()

    for l in range(blocks):
        loads[l].wait()

        def turn(k, carry):
            at = pl.ds(pl.multiple_of(k * rc, 128), rc)
            high, low = split(dip_full[l * rc : (l + 1) * rc, at])
            dip_cat[2 * l * rc : (2 * l + 1) * rc, at] = high
            dip_cat[(2 * l + 1) * rc : (2 * l + 2) * rc, at] = low
            base = k * depth + 2 * l * rc
            dip_turn[pl.ds(pl.multiple_of(base, 128), rc), :] = high.T
            dip_turn[pl.ds(pl.multiple_of(base + rc, 128), rc), :] = low.T
            return carry

        lax.fori_loop(0, sectors, turn, 0)

    @pl.when(has_below)
    def _():
        share.wait_recv()

    @pl.when(has_above)
    def _():
        share.wait_send()

    reach = -(-(nc + 2 * ch) // 128) * 128
    fill = jnp.zeros((ch, reach - side), f32)
    mixed_rows = []
    for l in range(blocks):
        upward = jnp.concatenate([pairs[l + 1, 0:ch, :], fill], axis=1)
        downward = jnp.concatenate([pairs[l].T[0:ch], fill], axis=1)
        upward = pltpu.roll(upward, (l + 2) * ch, 1)
        if l:
            downward = pltpu.roll(downward, l * ch, 1)
        mixed_rows.append((upward + downward)[:, 0 : nc + 2 * ch])
    mh, ml = split(jnp.concatenate(mixed_rows, axis=0))
    mix_split[0:nc, :] = mh
    mix_split[nc : 2 * nc, :] = ml
    for p in range(2):
        states[4 * p].wait()
        states[4 * p + 3].wait()

    row_block = lax.broadcasted_iota(jnp.int32, (rows, 1), 0) // 2
    low_lane = ch + ch * (lax.broadcasted_iota(jnp.int32, (rows, ext), 0) // 2)
    lane_of = lax.broadcasted_iota(jnp.int32, (rows, ext), 1)
    own_lanes = (lane_of >= low_lane) & (lane_of < low_lane + ch)

    def eye(count, shift):
        return (
            lax.broadcasted_iota(jnp.int32, (count, ext), 0) + shift
            == lax.broadcasted_iota(jnp.int32, (count, ext), 1)
        )

    def to_row(col):
        return jnp.sum(jnp.where(eye(nc, ch), col, 0.0), axis=0, keepdims=True)

    def to_col(row, count, shift):
        return jnp.sum(jnp.where(eye(count, shift), row, 0.0), axis=1, keepdims=True)

    def spread(v, first, count):
        high, low = halves(v)
        zero = jnp.zeros_like(v)
        top, bottom = [], []
        for l in range(first, first + count):
            mine = row_block == l
            h = jnp.where(mine, high, 0.0)
            top += [h, h]
            bottom += [jnp.where(mine, low, 0.0), zero]
        return jnp.concatenate(
            [jnp.concatenate(top, axis=1), jnp.concatenate(bottom, axis=1)], axis=0
        ).astype(bf16)

    def stacked(v):
        high, low = halves(v)
        return jnp.concatenate(
            [
                jnp.concatenate([high, high], axis=1),
                jnp.concatenate([low, jnp.zeros_like(low)], axis=1),
            ],
            axis=0,
        ).astype(bf16)

    def fold(r):
        return r[:rows] + r[rows:]

    def edge_sends(st, f):
        def three(cond, src, dst, sem, send, sector):
            @pl.when(cond)
            def _():
                f(remote(src, dst(0), send.at[0], sem.at[st, 0], z, sector))

                @pl.when(has_below)
                def _():
                    f(remote(src, dst(2), send.at[1], sem.at[st, 2], z - 1, sector))

                @pl.when(has_above)
                def _():
                    f(remote(src, dst(1), send.at[2], sem.at[st, 1], z + 1, sector))

        three(
            me > 0,
            edge_out.at[st, pl.ds(0, 2)],
            lambda o: right_in.at[st, o, pl.ds(0, 2)],
            sem_right,
            sem_e_send.at[0],
            me - 1,
        )
        three(
            me < sectors - 1,
            edge_out.at[st + SLOTS, pl.ds(0, 2)],
            lambda o: left_in.at[st, o, pl.ds(0, 2)],
            sem_left,
            sem_e_send.at[1],
            me + 1,
        )

    def surf_sends(st, f):
        src = surf_in.at[st, 0, me, pl.ds(0, 2)]

        @pl.when(me > 0)
        def _():
            f(remote(src, src, sem_surf_send.at[0], sem_surf.at[st, 0], z, 0))

        @pl.when(has_below)
        def _():
            dst = surf_in.at[st, 2, me, pl.ds(0, 2)]
            f(remote(src, dst, sem_surf_send.at[1], sem_surf.at[st, 2], z - 1, 0))

        @pl.when(has_above)
        def _():
            dst = surf_in.at[st, 1, me, pl.ds(0, 2)]
            f(remote(src, dst, sem_surf_send.at[2], sem_surf.at[st, 1], z + 1, 0))

    def point_sends(st, f):
        @pl.when(me == 0)
        def _():
            src = point_in.at[st, pl.ds(0, 2)]
            for k in range(1, sectors):
                f(remote(src, src, sem_point_send.at[k], sem_point.at[st], z, k))

    def edge_waits(sl):
        def each(f):
            f(0)

            @pl.when(has_below)
            def _():
                f(1)

            @pl.when(has_above)
            def _():
                f(2)

        @pl.when(me > 0)
        def _():
            each(lambda o: wait(left_in.at[sl, o, pl.ds(0, 2)], sem_left.at[sl, o]))

        @pl.when(me < sectors - 1)
        def _():
            each(lambda o: wait(right_in.at[sl, o, pl.ds(0, 2)], sem_right.at[sl, o]))

        @pl.when(me == 0)
        def _():
            each(
                lambda o: wait(
                    surf_in.at[sl, o, pl.ds(1 if o == 0 else 0, sectors - (o == 0)), pl.ds(0, 2)],
                    sem_surf.at[sl, o],
                )
            )

    def edge_rows(sl, o):
        total_b = surf_in[sl, o, 0]
        for k in range(1, sectors):
            total_b = total_b + surf_in[sl, o, k]
        left = jnp.where(me == 0, total_b, left_in[sl, o])
        right = jnp.where(me == sectors - 1, 0.0, right_in[sl, o])
        if o == 1:
            left, right = jnp.where(has_below, left, 0.0), jnp.where(has_below, right, 0.0)
        if o == 2:
            left, right = jnp.where(has_above, left, 0.0), jnp.where(has_above, right, 0.0)
        return left, right

    lane = lax.broadcasted_iota(jnp.int32, (1, 128), 1)

    def scales(t):
        order = lax.rem(t, ORDER)
        factor = time_step / (order + 1).astype(f32)
        return factor * kinetic_scale, -factor * kinetic_scale

    def correct_own(t, par, refresh):
        sl = lax.rem(t, SLOTS)
        left, right = edge_rows(sl, 0)
        for d, scale in ((1, scales(t)[0]), (0, scales(t)[1])):
            first = jnp.where(lane == 0, scale * to_col(left[1 - d : 2 - d], nc, ch), 0.0)
            last = jnp.where(lane == 127, scale * to_col(right[1 - d : 2 - d], nc, ch), 0.0)
            outer_out[d, :, 0:128] += first
            outer_out[d, :, nr - 128 : nr] += last
            if refresh:
                grid[par, d, own, 0:128] += first
                grid[par, d, own, nr - 128 : nr] += last

    def apply(t, carry):
        par = lax.rem(t, 2)
        nxt = 1 - par
        st = lax.rem(t, SLOTS)
        order = lax.rem(t, ORDER)
        strength = field_ref[lax.div(t, ORDER)]
        factor = time_step / (order + 1).astype(f32)
        last = order == ORDER - 1

        c = term[...]
        shifted = pltpu.roll(c, rows - 2, 0)
        peer_in[par, me] = shifted
        first_out[par] = c
        copies = []
        for s in range(sectors - 1, 0, -1):
            here = peer_in.at[par, me, pl.ds(0, near)]
            copies.append(
                remote(here, here, sem_a_send.at[s], sem_a_recv.at[par, s], z, partner(s))
            )
        z_copies = [
            remote(
                first_out.at[par, pl.ds(0, 2)],
                above_in.at[par, me, pl.ds(0, 2)],
                sem_z_send.at[s],
                sem_z_recv.at[par, s],
                z - 1,
                partner(s),
            )
            for s in range(sectors - 1, -1, -1)
        ]

        @pl.when(has_below)
        def _():
            for copy in z_copies:
                copy.start()

        for copy in copies:
            copy.start()

        b = fold(dot(stacked(c), surf_turn[...]))
        b = jnp.where(own_lanes, b, 0.0)
        total_b = b
        for l in range(1, blocks):
            total_b = total_b + pltpu.roll(b, 2 * l, 0)
        surf_in[st, 0, me] = total_b
        surf_sends(st, lambda copy: copy.start())

        lhs = stacked(c)
        y_copies, b_copies = [], []
        for s in range(sectors - 1, -1, -1):
            to = partner(s)
            at = pl.ds(pl.multiple_of(to * rc, 128), rc)
            back = jnp.zeros((rows, rc), f32)
            for l in range(blocks):
                r = fold(dot(lhs, dip_cat[2 * l * rc : 2 * (l + 1) * rc, at]))
                back = jnp.where(row_block == l, r, back)
            if s:
                part_out[s] = back
                b_copies.append(
                    remote(
                        part_out.at[s, pl.ds(0, near)],
                        part_in.at[par, me, pl.ds(0, near)],
                        sem_b_send.at[s],
                        sem_b_recv.at[par, s],
                        z,
                        to,
                    )
                )
            else:
                part_in[par, me] = back
            far_out[s] = pltpu.roll(back, 2, 0)
            y_copies.append(
                remote(
                    far_out.at[s, pl.ds(0, 2)],
                    below_in.at[par, me, pl.ds(0, 2)],
                    sem_y_send.at[s],
                    sem_y_recv.at[par, s],
                    z + 1,
                    to,
                )
            )
            if s % 2 == 0:

                @pl.when(has_above)
                def _():
                    for copy in y_copies[-2:]:
                        copy.start()

                for copy in b_copies[-2:] if s else b_copies[-1:]:
                    copy.start()

        @pl.when(t > 0)
        def _():
            edge_waits(lax.rem(t + SLOTS - 1, SLOTS))
            correct_own(t - 1, par, True)

        for e in range(2):
            edges = []
            for p in range(2):
                x = grid[par, p, own, nr - 128 : nr] if e else grid[par, p, own, 0:128]
                edges.append(to_row(x[:, 127:128] if e else x[:, 0:1]))
            edges.append(jnp.zeros((6, ext), f32))
            edge_out[st + e * SLOTS] = jnp.concatenate(edges, axis=0)

        @pl.when(me == 0)
        def _():
            point_in[st] = edge_out[st]

        point_sends(st, lambda copy: copy.start())
        edge_sends(st, lambda copy: copy.start())

        def unit(q):
            p = lax.rem(t + 1 + q, 2)
            imag = p == 1
            up, down = channel_copies(par, p)

            @pl.when(has_below)
            def _():
                up.wait_recv()

            @pl.when(has_above)
            def _():
                down.wait_recv()

            @pl.when(t > 0)
            def _():
                sl = lax.rem(t + SLOTS - 1, SLOTS)
                one, zero = scales(t - 1)
                scale = jnp.where(imag, one, zero)
                for o, start, shift in ((1, 0, nc), (2, ch + nc, ch)):
                    left, right = edge_rows(sl, o)
                    left = jnp.where(imag, left[0:1], left[1:2])
                    right = jnp.where(imag, right[0:1], right[1:2])
                    at = pl.ds(start, ch)
                    grid[par, p, at, 0:128] += jnp.where(
                        lane == 0, scale * to_col(left, ch, shift), 0.0
                    )
                    grid[par, p, at, nr - 128 : nr] += jnp.where(
                        lane == 127, scale * to_col(right, ch, shift), 0.0
                    )

            gh, gl = split(grid[par, p])
            r = dot(mix_split[...], gh)
            coupled = r[:nc] + r[nc:] + dot(mix_split[0:nc, :], gl)
            x = grid[par, p, own, :]
            lanes = lax.broadcasted_iota(jnp.int32, (1, nr), 1)
            left = jnp.where(lanes == 0, 0.0, pltpu.roll(x, 1, 1))
            right = jnp.where(lanes == nr - 1, 0.0, pltpu.roll(x, nr - 1, 1))
            image = diag_ref[...] * x - kinetic_scale * (left + right) + strength * coupled
            value = jnp.where(imag, factor, -factor) * image
            acc = outer_out[1 - p] + value
            outer_out[1 - p] = acc
            value = jnp.where(last, acc, value)
            up_old, down_old = channel_copies(par, 1 - p)

            @pl.when(has_above)
            def _():
                up_old.wait_send()

            @pl.when(has_below)
            def _():
                down_old.wait_send()

            grid[nxt, 1 - p, own, :] = value
            halo_out[1 - p, 0] = value[nc - ch : nc]
            halo_out[1 - p, 1] = value[0:ch]
            up_new, down_new = channel_copies(nxt, 1 - p)

            @pl.when(jnp.logical_and(has_above, t < STEPS * ORDER - 1))
            def _():
                up_new.start()

            @pl.when(jnp.logical_and(has_below, t < STEPS * ORDER - 1))
            def _():
                down_new.start()

        def take(groups, first, count):
            for s in groups:
                if s and first == 0:
                    wait(peer_in.at[par, source(s), pl.ds(0, near)], sem_a_recv.at[par, s])
            total = jnp.zeros((rows, rc), f32)
            for group in (groups[0::2], groups[1::2]):
                sums = [None] * count
                for s in group:
                    k = source(s)
                    if first:
                        left = stacked(pltpu.roll(above_in[par, k], rows - 2, 0))
                    else:
                        left = stacked(peer_in[par, k])
                    for i in range(count):
                        base = k * depth + 2 * (first + i) * rc
                        at = pl.ds(pl.multiple_of(base, 128), 2 * rc)
                        part = dot(left, dip_turn[at, :])
                        sums[i] = part if sums[i] is None else sums[i] + part
                for i in range(count):
                    total = total + jnp.where(row_block == first + i, fold(sums[i]), 0.0)
            return total

        unit(0)
        ahead = take([0, 1], 0, blocks - 1)
        middle = list(range(2, sectors * 3 // 4))
        tail = list(range(sectors * 3 // 4, sectors))
        unit(1)
        ahead = ahead + take(middle, 0, blocks - 1)
        ahead = ahead + take(tail, 0, blocks - 1)

        @pl.when(me > 0)
        def _():
            wait(point_in.at[st, pl.ds(0, 2)], sem_point.at[st])

        point = jnp.concatenate([point_in[st, 0:2]] * blocks, axis=0)
        surf = fold(dot(stacked(jnp.where(own_lanes, point, 0.0)), surf_cat[...]))

        for s in range(1, sectors):
            wait(part_in.at[par, source(s), pl.ds(0, near)], sem_b_recv.at[par, s])
        behind = part_in[par, 0]
        for k in range(1, sectors):
            behind = behind + part_in[par, k]

        @pl.when(has_above)
        def _():
            for s in range(sectors):
                wait(above_in.at[par, source(s), pl.ds(0, 2)], sem_z_recv.at[par, s])

        ahead = ahead + take(list(range(sectors)), blocks - 1, 1)

        @pl.when(has_below)
        def _():
            for s in range(sectors):
                wait(below_in.at[par, source(s), pl.ds(0, 2)], sem_y_recv.at[par, s])

        far = below_in[par, 0]
        for k in range(1, sectors):
            far = far + below_in[par, k]
        behind = jnp.where(row_block == 0, far, pltpu.roll(behind, 2, 0))
        image = live_ref[...] * (
            energy_rows[...] * c + strength * (ahead + behind) - kinetic_scale * surf
        )
        even = lax.rem(lax.broadcasted_iota(jnp.int32, (rows, 1), 0), 2) == 0
        value = factor * jnp.where(
            even, pltpu.roll(image, rows - 1, 0), -pltpu.roll(image, 1, 0)
        )
        acc = total_inner[...] + value
        total_inner[...] = acc
        term[...] = jnp.where(last, acc, value)

        for copy in copies + b_copies:
            copy.wait_send()

        @pl.when(has_below)
        def _():
            for copy in z_copies:
                copy.wait_send()

        @pl.when(has_above)
        def _():
            for copy in y_copies:
                copy.wait_send()

        surf_sends(st, lambda copy: copy.wait_send())
        point_sends(st, lambda copy: copy.wait_send())
        edge_sends(st, lambda copy: copy.wait_send())
        return carry

    count = STEPS * ORDER
    lax.fori_loop(0, count, apply, 0)
    edge_waits((count - 1) % SLOTS)
    correct_own(jnp.int32(count - 1), 0, False)
    final = total_inner[...]
    for p in range(2):
        inner_out[p] = jnp.concatenate(
            [final[2 * l + p : 2 * l + p + 1] for l in range(blocks)], axis=0
        )


def local(
    planes,
    sectors,
    inner_state,
    outer_state,
    energies,
    dipole,
    surface,
    thresholds,
    coupling_coef,
    coupling_pattern,
    block_sizes,
    field_strength,
):
    blocks, rc, total = dipole.shape
    ch = coupling_coef.shape[1]
    nc, nr = outer_state.shape[1:]
    rows = 2 * blocks
    ext = -(-(nc + 2 * ch) // 128) * 128
    vmem = pl.BlockSpec(memory_space=pltpu.VMEM)
    hbm = pl.BlockSpec(memory_space=pltpu.HBM)
    dma = pltpu.SemaphoreType.DMA
    smem = pl.BlockSpec(memory_space=pltpu.SMEM)
    side = -(-ch // 128) * 128
    return pl.pallas_call(
        functools.partial(kernel, planes, sectors, ch),
        out_shape=(
            jax.ShapeDtypeStruct((2, blocks, rc), f32),
            jax.ShapeDtypeStruct((2, nc, nr), f32),
        ),
        in_specs=[vmem, hbm, vmem, hbm] + [vmem] * 4 + [smem] * 2,
        out_specs=(vmem, vmem),
        scratch_shapes=[
            pltpu.VMEM((blocks * rc, total), f32),
            pltpu.VMEM((2 * blocks * rc, total), bf16),
            pltpu.VMEM((2 * blocks * total, rc), bf16),
            pltpu.VMEM((2 * ext, rc), bf16),
            pltpu.VMEM((2 * rc, ext), bf16),
            pltpu.VMEM((2 * nc, nc + 2 * ch), bf16),
            pltpu.VMEM((2, 2, nc + 2 * ch, nr), f32),
            pltpu.VMEM((2, 2, ch, nr), f32),
            pltpu.VMEM((rows, rc), f32),
            pltpu.VMEM((2, sectors, rows, rc), f32),
            pltpu.VMEM((2, rows, rc), f32),
            pltpu.VMEM((2, sectors, rows, rc), f32),
            pltpu.VMEM((sectors, rows, rc), f32),
            pltpu.VMEM((2, sectors, rows, rc), f32),
            pltpu.VMEM((sectors, rows, rc), f32),
            pltpu.VMEM((2, sectors, rows, rc), f32),
            pltpu.VMEM((blocks + 1, side, side), f32),
            pltpu.VMEM((rows, rc), f32),
            pltpu.VMEM((rows, rc), f32),
            pltpu.VMEM((rows, rc), f32),
            pltpu.VMEM((nc, 1), f32),
            pltpu.VMEM((2 * SLOTS, 8, ext), f32),
            pltpu.VMEM((SLOTS, 3, 8, ext), f32),
            pltpu.VMEM((SLOTS, 3, 8, ext), f32),
            pltpu.VMEM((SLOTS, 3, sectors, 8, ext), f32),
            pltpu.VMEM((SLOTS, 8, ext), f32),
            dma((blocks,)), dma((8,)), dma(()), dma(()),
            dma((sectors,)), dma((2, sectors)),
            dma((sectors,)), dma((2, sectors)),
            dma((sectors,)), dma((2, sectors)),
            dma((sectors,)), dma((2, sectors)),
            dma((2,)), dma((2, 2)), dma((2,)), dma((2, 2)),
            dma((2, 3)), dma((SLOTS, 3)), dma((SLOTS, 3)),
            dma((3,)), dma((SLOTS, 3)),
            dma((sectors,)), dma((SLOTS,)),
        ],
        compiler_params=pltpu.CompilerParams(
            collective_id=0, has_side_effects=True, vmem_limit_bytes=56 * 1024 * 1024
        ),
    )(
        inner_state,
        outer_state,
        energies,
        dipole.reshape(blocks * rc, total),
        surface.reshape(nc, rc),
        thresholds.reshape(1, nc),
        coupling_coef,
        coupling_pattern,
        block_sizes,
        field_strength,
    )
def solution(mesh):
    placed = (
        P(None, "inner", "outer"),
        P(None, "inner", "outer"),
        P("inner", "outer"),
        P("inner", "outer", None),
        P("inner", None, "outer"),
        P("inner"),
        P("inner", None, None),
        P("inner", None, None),
        P("inner"),
        P(),
    )
    return jax.shard_map(
        functools.partial(local, mesh.shape["inner"], mesh.shape["outer"]),
        mesh=mesh,
        in_specs=placed,
        out_specs=(P(None, "inner", "outer"), P(None, "inner", "outer")),
        check_vma=False,
    )
```

```python
import functools

import jax
import jax.numpy as jnp
from jax import lax
from jax.experimental import pallas as pl
from jax.experimental.pallas import tpu as pltpu
from jax.sharding import PartitionSpec as P

STEPS = 2
ORDER = 4

kinetic_scale = 3.125
time_step = 0.1

MESH = pl.DeviceIdType.MESH
f32 = jnp.float32
bf16 = jnp.bfloat16
NN = (((1,), (0,)), ((), ()))
SLOTS = 4


def halves(x):
    high = x.astype(bf16).astype(f32)
    return high, x - high


def split(x):
    high = x.astype(bf16)
    return high, (x - high.astype(f32)).astype(bf16)


def dot(a, b):
    return lax.dot_general(a, b, NN, preferred_element_type=f32)


def kernel(
    planes,
    sectors,
    ch,
    inner_hbm,
    outer_hbm,
    energy_hbm,
    dipole_hbm,
    surface_hbm,
    threshold_hbm,
    coef_hbm,
    pattern_hbm,
    size_hbm,
    field_hbm,
    inner_out,
    outer_out,
    inner_ref,
    energy_ref,
    surface_ref,
    threshold_ref,
    coef_ref,
    pattern_ref,
    size_ref,
    field_ref,
    sem_small,
    dip_full,
    dip_cat,
    dip_turn,
    surf_cat,
    surf_turn,
    mix_split,
    grid,
    halo_out,
    term,
    peer_in,
    first_out,
    above_in,
    part_out,
    part_in,
    far_out,
    below_in,
    pairs,
    live_ref,
    energy_rows,
    total_inner,
    diag_ref,
    raw_rows,
    edge_out,
    left_in,
    right_in,
    surf_in,
    point_in,
    sem_load,
    sem_outer,
    sem_g_send,
    sem_g_recv,
    sem_a_send,
    sem_a_recv,
    sem_z_send,
    sem_z_recv,
    sem_b_send,
    sem_b_recv,
    sem_y_send,
    sem_y_recv,
    sem_up_send,
    sem_up_recv,
    sem_down_send,
    sem_down_recv,
    sem_e_send,
    sem_left,
    sem_right,
    sem_surf_send,
    sem_surf,
    sem_point_send,
    sem_point,
):
    z = lax.axis_index("inner")
    me = lax.axis_index("outer")
    blocks, rc = energy_hbm.shape
    rows = 2 * blocks
    nc, nr = grid.shape[2] - 2 * ch, grid.shape[3]
    ext = edge_out.shape[2]
    depth = 2 * blocks * rc
    near = rows - 2
    has_below = z > 0
    has_above = z < planes - 1
    power = sectors & (sectors - 1) == 0

    def partner(s):
        if not power:
            return lax.rem(me + s, sectors)
        to, bit = me, 1
        while bit < sectors:
            if s & bit:
                to = to + bit * (1 - 2 * ((me // bit) % 2))
            bit *= 2
        return to

    def source(s):
        return partner(s) if power else lax.rem(me + sectors - s, sectors)

    def remote(src, dst, send, recv, plane, sector):
        return pltpu.make_async_remote_copy(
            src_ref=src,
            dst_ref=dst,
            send_sem=send,
            recv_sem=recv,
            device_id={"inner": plane, "outer": sector},
            device_id_type=MESH,
        )

    def wait(ref, sem):
        pltpu.make_async_copy(ref, ref, sem).wait()

    barrier = pltpu.get_barrier_semaphore()

    def greet(plane, s):
        pl.semaphore_signal(
            barrier,
            inc=1,
            device_id={"inner": plane, "outer": partner(s)},
            device_id_type=MESH,
        )

    for s in range(sectors - 1, 0, -1):
        greet(z, s)

    @pl.when(has_below)
    def _():
        for s in range(sectors - 1, -1, -1):
            greet(z - 1, s)

    @pl.when(has_above)
    def _():
        for s in range(sectors - 1, -1, -1):
            greet(z + 1, s)

    own = pl.ds(ch, nc)
    small_loads = [
        pltpu.make_async_copy(src, dst, sem_small.at[i])
        for i, (src, dst) in enumerate(
            (
                (inner_hbm, inner_ref),
                (size_hbm, size_ref),
                (coef_hbm, coef_ref),
                (pattern_hbm, pattern_ref),
                (surface_hbm, surface_ref),
                (threshold_hbm, threshold_ref),
                (energy_hbm, energy_ref),
                (field_hbm, field_ref),
            )
        )
    ]
    for load in small_loads:
        load.start()
    states = []
    for p in range(2):
        states.append(
            pltpu.make_async_copy(outer_hbm.at[p], grid.at[0, p, own, :], sem_outer.at[p])
        )
        states.append(
            pltpu.make_async_copy(
                outer_hbm.at[p, pl.ds(nc - ch, ch)], halo_out.at[p, 0], sem_outer.at[2 + p]
            )
        )
        states.append(
            pltpu.make_async_copy(
                outer_hbm.at[p, pl.ds(0, ch)], halo_out.at[p, 1], sem_outer.at[4 + p]
            )
        )
        states.append(
            pltpu.make_async_copy(outer_hbm.at[p], outer_out.at[p], sem_outer.at[6 + p])
        )
    for p in (1, 0):
        states[4 * p + 1].start()
        states[4 * p + 2].start()
    loads = [
        pltpu.make_async_copy(
            dipole_hbm.at[pl.ds(l * rc, rc)], dip_full.at[pl.ds(l * rc, rc)], sem_load.at[l]
        )
        for l in range(blocks)
    ]
    for load in loads:
        load.start()
    for p in range(2):
        states[4 * p].start()
        states[4 * p + 3].start()

    raw_rows[...] = jnp.zeros_like(raw_rows)

    @pl.when(z == 0)
    def _():
        below_in[...] = jnp.zeros_like(below_in)
        grid[:, :, 0:ch, :] = jnp.zeros((2, 2, ch, nr), f32)

    @pl.when(z == planes - 1)
    def _():
        above_in[...] = jnp.zeros_like(above_in)
        grid[:, :, ch + nc : 2 * ch + nc, :] = jnp.zeros((2, 2, ch, nr), f32)

    def channel_copies(slot, p):
        up = remote(
            halo_out.at[p, 0],
            grid.at[slot, p, pl.ds(0, ch), :],
            sem_up_send.at[p],
            sem_up_recv.at[slot, p],
            z + 1,
            me,
        )
        down = remote(
            halo_out.at[p, 1],
            grid.at[slot, p, pl.ds(ch + nc, ch), :],
            sem_down_send.at[p],
            sem_down_recv.at[slot, p],
            z - 1,
            me,
        )
        return up, down

    for load in small_loads:
        load.wait()

    side = pairs.shape[1]
    for l in range(blocks + 1):
        pairs[l, ch:side, :] = jnp.zeros((side - ch, side), f32)
    for l in range(blocks):
        pairs[l + 1, 0:ch, :] = jnp.zeros((ch, side), f32)
        pairs[l + 1, 0:ch, 0:ch] = coef_ref[l] * pattern_ref[l].astype(f32)

    @pl.when(z == 0)
    def _():
        pairs[0, 0:ch, :] = jnp.zeros((ch, side), f32)

    share = remote(
        pairs.at[blocks, pl.ds(0, ch), :],
        pairs.at[0, pl.ds(0, ch), :],
        sem_g_send,
        sem_g_recv,
        z + 1,
        me,
    )

    order_of = [(l, p) for l in range(blocks) for p in range(2)]
    position = me * rc + lax.broadcasted_iota(jnp.int32, (1, rc), 1)
    live_ref[...] = jnp.concatenate(
        [jnp.where(position < size_ref[:, l : l + 1], 1.0, 0.0) for l, p in order_of], axis=0
    )
    energy_rows[...] = jnp.concatenate([energy_ref[l : l + 1, :] for l, p in order_of], axis=0)
    term[...] = live_ref[...] * jnp.concatenate(
        [inner_ref[p, l : l + 1, :] for l, p in order_of], axis=0
    )
    total_inner[...] = term[...]

    small = lax.broadcasted_iota(jnp.int32, (nc, nc), 0) == lax.broadcasted_iota(
        jnp.int32, (nc, nc), 1
    )
    diag_ref[...] = 2.0 * kinetic_scale + jnp.sum(
        jnp.where(small, threshold_ref[...], 0.0), axis=1, keepdims=True
    )

    surface_ext = jnp.concatenate(
        [
            jnp.zeros((ch, rc), f32),
            surface_ref[...],
            jnp.zeros((ext - ch - nc, rc), f32),
        ],
        axis=0,
    )
    sh, sl = split(surface_ext)
    surf_cat[0:ext, :] = sh
    surf_cat[ext : 2 * ext, :] = sl
    surf_turn[0:rc, :] = sh.T
    surf_turn[rc : 2 * rc, :] = sl.T

    waits = (sectors - 1) + sectors * (
        jnp.where(has_below, 1, 0) + jnp.where(has_above, 1, 0)
    )
    pl.semaphore_wait(barrier, waits)

    @pl.when(has_above)
    def _():
        share.start()

    for p in (1, 0):
        states[4 * p + 1].wait()
        states[4 * p + 2].wait()
        up, down = channel_copies(0, p)

        @pl.when(has_above)
        def _():
            up.start()

        @pl.when(has_below)
        def _():
            down.start()

    count = STEPS * ORDER
    row_block = lax.broadcasted_iota(jnp.int32, (rows, 1), 0) // 2
    low_lane = ch + ch * (lax.broadcasted_iota(jnp.int32, (rows, ext), 0) // 2)
    lane_of = lax.broadcasted_iota(jnp.int32, (rows, ext), 1)
    own_lanes = (lane_of >= low_lane) & (lane_of < low_lane + ch)

    def eye(count, shift):
        return (
            lax.broadcasted_iota(jnp.int32, (count, ext), 0) + shift
            == lax.broadcasted_iota(jnp.int32, (count, ext), 1)
        )

    def to_row(col):
        return jnp.sum(jnp.where(eye(nc, ch), col, 0.0), axis=0, keepdims=True)

    def to_col(row, count, shift):
        return jnp.sum(jnp.where(eye(count, shift), row, 0.0), axis=1, keepdims=True)

    def spread(v, first, count):
        high, low = halves(v)
        zero = jnp.zeros_like(v)
        top, bottom = [], []
        for l in range(first, first + count):
            mine = row_block == l
            h = jnp.where(mine, high, 0.0)
            top += [h, h]
            bottom += [jnp.where(mine, low, 0.0), zero]
        return jnp.concatenate(
            [jnp.concatenate(top, axis=1), jnp.concatenate(bottom, axis=1)], axis=0
        ).astype(bf16)

    def stacked(v):
        high, low = halves(v)
        return jnp.concatenate(
            [
                jnp.concatenate([high, high], axis=1),
                jnp.concatenate([low, jnp.zeros_like(low)], axis=1),
            ],
            axis=0,
        ).astype(bf16)

    def fold(r):
        return r[:rows] + r[rows:]

    def edge_sends(st, f):
        def three(cond, src, dst, sem, send, sector):
            @pl.when(cond)
            def _():
                f(remote(src, dst(0), send.at[0], sem.at[st, 0], z, sector))

                @pl.when(has_below)
                def _():
                    f(remote(src, dst(2), send.at[1], sem.at[st, 2], z - 1, sector))

                @pl.when(has_above)
                def _():
                    f(remote(src, dst(1), send.at[2], sem.at[st, 1], z + 1, sector))

        three(
            me > 0,
            edge_out.at[st, pl.ds(0, 2)],
            lambda o: right_in.at[st, o, pl.ds(0, 2)],
            sem_right,
            sem_e_send.at[0],
            me - 1,
        )
        three(
            me < sectors - 1,
            edge_out.at[st + SLOTS, pl.ds(0, 2)],
            lambda o: left_in.at[st, o, pl.ds(0, 2)],
            sem_left,
            sem_e_send.at[1],
            me + 1,
        )

    def surf_sends(st, f):
        src = surf_in.at[st, 0, me, pl.ds(0, 2)]

        @pl.when(me > 0)
        def _():
            f(remote(src, src, sem_surf_send.at[0], sem_surf.at[st, 0], z, 0))

        @pl.when(has_below)
        def _():
            dst = surf_in.at[st, 2, me, pl.ds(0, 2)]
            f(remote(src, dst, sem_surf_send.at[1], sem_surf.at[st, 2], z - 1, 0))

        @pl.when(has_above)
        def _():
            dst = surf_in.at[st, 1, me, pl.ds(0, 2)]
            f(remote(src, dst, sem_surf_send.at[2], sem_surf.at[st, 1], z + 1, 0))

    def point_sends(st, f):
        @pl.when(me == 0)
        def _():
            src = point_in.at[st, pl.ds(0, 2)]
            for k in range(1, sectors):
                f(remote(src, src, sem_point_send.at[k], sem_point.at[st], z, k))

    def edge_wait(sl, o):
        @pl.when(me > 0)
        def _():
            wait(left_in.at[sl, o, pl.ds(0, 2)], sem_left.at[sl, o])

        @pl.when(me < sectors - 1)
        def _():
            wait(right_in.at[sl, o, pl.ds(0, 2)], sem_right.at[sl, o])

        @pl.when(me == 0)
        def _():
            first = 1 if o == 0 else 0
            wait(
                surf_in.at[sl, o, pl.ds(first, sectors - first), pl.ds(0, 2)],
                sem_surf.at[sl, o],
            )

    def edge_waits_beyond(sl):
        @pl.when(has_below)
        def _():
            edge_wait(sl, 1)

        @pl.when(has_above)
        def _():
            edge_wait(sl, 2)

    def edge_rows(sl, o):
        total_b = surf_in[sl, o, 0]
        for k in range(1, sectors):
            total_b = total_b + surf_in[sl, o, k]
        left = jnp.where(me == 0, total_b, left_in[sl, o])
        right = jnp.where(me == sectors - 1, 0.0, right_in[sl, o])
        if o == 1:
            left, right = jnp.where(has_below, left, 0.0), jnp.where(has_below, right, 0.0)
        if o == 2:
            left, right = jnp.where(has_above, left, 0.0), jnp.where(has_above, right, 0.0)
        return left, right

    lane = lax.broadcasted_iota(jnp.int32, (1, 128), 1)

    def scales(t):
        order = lax.rem(t, ORDER)
        factor = time_step / (order + 1).astype(f32)
        return factor * kinetic_scale, -factor * kinetic_scale

    def correct_own(t, par, refresh):
        valid = t >= 0
        sl = lax.rem(t + SLOTS, SLOTS)
        t = jnp.maximum(t, 0)
        left, right = [jnp.where(valid, row, 0.0) for row in edge_rows(sl, 0)]
        for d, scale in ((1, scales(t)[0]), (0, scales(t)[1])):
            first = jnp.where(lane == 0, scale * to_col(left[1 - d : 2 - d], nc, ch), 0.0)
            last = jnp.where(lane == 127, scale * to_col(right[1 - d : 2 - d], nc, ch), 0.0)
            outer_out[d, :, 0:128] += first
            outer_out[d, :, nr - 128 : nr] += last
            if refresh:
                grid[par, d, own, 0:128] += first
                grid[par, d, own, nr - 128 : nr] += last

    def a_copies(par):
        here = peer_in.at[par, me, pl.ds(0, near)]
        return [
            remote(here, here, sem_a_send.at[s], sem_a_recv.at[par, s], z, partner(s))
            for s in range(sectors - 1, 0, -1)
        ]

    def z_copies(par):
        return [
            remote(
                first_out.at[par, pl.ds(0, 2)],
                above_in.at[par, me, pl.ds(0, 2)],
                sem_z_send.at[s],
                sem_z_recv.at[par, s],
                z - 1,
                partner(s),
            )
            for s in range(sectors - 1, -1, -1)
        ]

    def b_copy(par, s):
        return remote(
            part_out.at[s, pl.ds(0, near)],
            part_in.at[par, me, pl.ds(0, near)],
            sem_b_send.at[s],
            sem_b_recv.at[par, s],
            z,
            partner(s),
        )

    def y_copy(par, s):
        return remote(
            far_out.at[s, pl.ds(0, 2)],
            below_in.at[par, me, pl.ds(0, 2)],
            sem_y_send.at[s],
            sem_y_recv.at[par, s],
            z + 1,
            partner(s),
        )

    def send_state(t):
        par = lax.rem(t, 2)
        c = term[...]
        first_out[par] = c
        peer_in[par, me] = pltpu.roll(c, rows - 2, 0)

        @pl.when(has_below)
        def _():
            for copy in z_copies(par):
                copy.start()

        for copy in a_copies(par):
            copy.start()

    row_of = lax.broadcasted_iota(jnp.int32, (8, 1), 0)

    def send_edges(t):
        st = lax.rem(t, SLOTS)
        edge_out[st] = raw_rows[0]
        edge_out[st + SLOTS] = raw_rows[1]

        @pl.when(t > 0)
        def _():
            sl = lax.rem(t + SLOTS - 1, SLOTS)
            edge_wait(sl, 0)
            one, zero = scales(t - 1)
            scale = jnp.where(row_of == 0, zero, one)
            for e, row in enumerate(edge_rows(sl, 0)):
                row = jnp.where(row_of == 0, pltpu.roll(row, 7, 0), pltpu.roll(row, 1, 0))
                edge_out[st + e * SLOTS] += scale * row

        @pl.when(me == 0)
        def _():
            point_in[st] = edge_out[st]

        point_sends(st, lambda copy: copy.start())
        edge_sends(st, lambda copy: copy.start())

    def send_back(t):
        par = lax.rem(t, 2)
        st = lax.rem(t, SLOTS)
        c = term[...]
        lhs = stacked(c)

        def product(l, s):
            at = pl.ds(pl.multiple_of(partner(s) * rc, 128), rc)
            return fold(dot(lhs, dip_cat[2 * l * rc : 2 * (l + 1) * rc, at]))

        def group(chosen):
            for s in chosen:
                far_out[s] = pltpu.roll(product(blocks - 1, s), 2, 0)
                back = jnp.zeros((rows, rc), f32)
                for l in range(blocks - 1):
                    back = jnp.where(row_block == l, product(l, s), back)
                if s:
                    part_out[s] = back
                else:
                    part_in[par, me] = back

            @pl.when(has_above)
            def _():
                for s in chosen:
                    y_copy(par, s).start()

            for s in chosen:
                if s:
                    b_copy(par, s).start()

        def send_surf():
            b = fold(dot(lhs, surf_turn[...]))
            b = jnp.where(own_lanes, b, 0.0)
            total_b = b
            for l in range(1, blocks):
                total_b = total_b + pltpu.roll(b, 2 * l, 0)
            surf_in[st, 0, me] = total_b
            surf_sends(st, lambda copy: copy.start())

        order = list(range(sectors - 1, -1, -1))
        group(order[: sectors // 2])
        send_surf()
        send_edges(t)
        group(order[sectors // 2 :])

    send_state(jnp.int32(0))
    for l in range(blocks):
        loads[l].wait()

        def divide(k, carry):
            at = pl.ds(pl.multiple_of(k * rc, 128), rc)
            high, low = split(dip_full[l * rc : (l + 1) * rc, at])
            dip_cat[2 * l * rc : (2 * l + 1) * rc, at] = high
            dip_cat[(2 * l + 1) * rc : (2 * l + 2) * rc, at] = low
            return carry

        lax.fori_loop(0, sectors, divide, 0, unroll=2)

    for p in range(2):
        states[4 * p].wait()
        states[4 * p + 3].wait()
        raw_rows[0, p : p + 1, :] = to_row(grid[0, p, own, 0:1])
        raw_rows[1, p : p + 1, :] = to_row(grid[0, p, own, nr - 1 : nr])
    send_back(jnp.int32(0))
    for l in range(blocks):

        def turn(k, carry):
            at = pl.ds(pl.multiple_of(k * rc, 128), rc)
            base = k * depth + 2 * l * rc
            high = dip_cat[2 * l * rc : (2 * l + 1) * rc, at]
            low = dip_cat[(2 * l + 1) * rc : (2 * l + 2) * rc, at]
            dip_turn[pl.ds(pl.multiple_of(base, 128), rc), :] = high.T
            dip_turn[pl.ds(pl.multiple_of(base + rc, 128), rc), :] = low.T
            return carry

        lax.fori_loop(0, sectors, turn, 0, unroll=2)

    @pl.when(has_below)
    def _():
        share.wait_recv()

    @pl.when(has_above)
    def _():
        share.wait_send()

    reach = -(-(nc + 2 * ch) // 128) * 128
    fill = jnp.zeros((ch, reach - side), f32)
    mixed_rows = []
    for l in range(blocks):
        upward = jnp.concatenate([pairs[l + 1, 0:ch, :], fill], axis=1)
        downward = jnp.concatenate([pairs[l].T[0:ch], fill], axis=1)
        upward = pltpu.roll(upward, (l + 2) * ch, 1)
        if l:
            downward = pltpu.roll(downward, l * ch, 1)
        mixed_rows.append((upward + downward)[:, 0 : nc + 2 * ch])
    mh, ml = split(jnp.concatenate(mixed_rows, axis=0))
    mix_split[0:nc, :] = mh
    mix_split[nc : 2 * nc, :] = ml

    def apply(t, carry):
        par = lax.rem(t, 2)
        nxt = 1 - par
        st = lax.rem(t, SLOTS)
        order = lax.rem(t, ORDER)
        step = lax.div(t, ORDER)
        strength = field_ref[:, 0:1]
        for i in range(1, STEPS):
            strength = jnp.where(step == i, field_ref[:, i : i + 1], strength)
        factor = time_step / (order + 1).astype(f32)
        last = order == ORDER - 1

        @pl.when(t > 0)
        def _():
            edge_waits_beyond(lax.rem(t + SLOTS - 1, SLOTS))

        def unit_wait(q):
            p = lax.rem(t + 1 + q, 2)
            up, down = channel_copies(par, p)
            up_old, down_old = channel_copies(par, 1 - p)

            @pl.when(has_below)
            def _():
                up.wait_recv()
                down_old.wait_send()

            @pl.when(has_above)
            def _():
                down.wait_recv()
                up_old.wait_send()

        def unit_start(q):
            p = lax.rem(t + 1 + q, 2)
            imag = p == 1
            past = jnp.maximum(t - 1, 0)
            sl = lax.rem(t + SLOTS - 1, SLOTS)
            one, zero = scales(past)
            scale = jnp.where(imag, one, zero)
            for o, start, shift in ((1, 0, nc), (2, ch + nc, ch)):
                left, right = [jnp.where(t > 0, row, 0.0) for row in edge_rows(sl, o)]
                left = jnp.where(imag, left[0:1], left[1:2])
                right = jnp.where(imag, right[0:1], right[1:2])
                at = pl.ds(start, ch)
                grid[par, p, at, 0:128] += jnp.where(
                    lane == 0, scale * to_col(left, ch, shift), 0.0
                )
                grid[par, p, at, nr - 128 : nr] += jnp.where(
                    lane == 127, scale * to_col(right, ch, shift), 0.0
                )
            gh, gl = split(grid[par, p])
            r = dot(mix_split[...], gh)
            return r[:nc] + r[nc:] + dot(mix_split[0:nc, :], gl)

        def unit_finish(q, coupled):
            p = lax.rem(t + 1 + q, 2)
            imag = p == 1
            x = grid[par, p, own, :]
            lanes = lax.broadcasted_iota(jnp.int32, (1, nr), 1)
            left = jnp.where(lanes == 0, 0.0, pltpu.roll(x, 1, 1))
            right = jnp.where(lanes == nr - 1, 0.0, pltpu.roll(x, nr - 1, 1))
            image = diag_ref[...] * x - kinetic_scale * (left + right) + strength * coupled
            value = jnp.where(imag, factor, -factor) * image
            acc = outer_out[1 - p] + value
            outer_out[1 - p] = acc
            value = jnp.where(last, acc, value)
            grid[nxt, 1 - p, own, :] = value
            raw_rows[0, pl.ds(1 - p, 1), :] = to_row(value[:, 0:1])
            raw_rows[1, pl.ds(1 - p, 1), :] = to_row(value[:, nr - 1 : nr])
            halo_out[1 - p, 0] = value[nc - ch : nc]
            halo_out[1 - p, 1] = value[0:ch]

        def unit_send(q):
            p = lax.rem(t + 1 + q, 2)
            up_new, down_new = channel_copies(nxt, 1 - p)

            @pl.when(jnp.logical_and(has_above, t < STEPS * ORDER - 1))
            def _():
                up_new.start()

            @pl.when(jnp.logical_and(has_below, t < STEPS * ORDER - 1))
            def _():
                down_new.start()

        def take_wait(group):
            for s in group:
                if s:
                    wait(peer_in.at[par, source(s), pl.ds(0, near)], sem_a_recv.at[par, s])

        def take(groups, first, count):
            total = jnp.zeros((rows, rc), f32)
            for group in (groups[0::2], groups[1::2]):
                sums = [None] * count
                for s in group:
                    k = source(s)
                    if first:
                        left = stacked(pltpu.roll(above_in[par, k], rows - 2, 0))
                    else:
                        left = stacked(peer_in[par, k])
                    for i in range(count):
                        base = k * depth + 2 * (first + i) * rc
                        at = pl.ds(pl.multiple_of(base, 128), 2 * rc)
                        part = dot(left, dip_turn[at, :])
                        sums[i] = part if sums[i] is None else sums[i] + part
                for i in range(count):
                    total = total + jnp.where(row_block == first + i, fold(sums[i]), 0.0)
            return total

        middle = list(range(2, sectors * 3 // 4))
        tail = list(range(sectors * 3 // 4, sectors))

        unit_wait(0)
        take_wait([0, 1])
        correct_own(t - 1, par, True)
        coupled = unit_start(0)
        ahead = take([0, 1], 0, blocks - 1)
        unit_finish(0, coupled)
        unit_send(0)

        unit_wait(1)
        take_wait(middle)
        coupled = unit_start(1)
        ahead = ahead + take(middle, 0, blocks - 1)
        unit_finish(1, coupled)
        unit_send(1)

        take_wait(tail)

        @pl.when(me > 0)
        def _():
            wait(point_in.at[st, pl.ds(0, 2)], sem_point.at[st])

        def far_wait(group):
            @pl.when(has_above)
            def _():
                for s in group:
                    wait(above_in.at[par, source(s), pl.ds(0, 2)], sem_z_recv.at[par, s])

        far_wait([0, 1] + middle)
        ahead = ahead + take(tail, 0, blocks - 1)
        point = jnp.concatenate([point_in[st, 0:2]] * blocks, axis=0)
        surf = fold(dot(stacked(jnp.where(own_lanes, point, 0.0)), surf_cat[...]))
        ahead = ahead + take([0, 1] + middle, blocks - 1, 1)

        for s in range(1, sectors):
            wait(part_in.at[par, source(s), pl.ds(0, near)], sem_b_recv.at[par, s])
        far_wait(tail)

        @pl.when(has_below)
        def _():
            for s in range(sectors):
                wait(below_in.at[par, source(s), pl.ds(0, 2)], sem_y_recv.at[par, s])

        ahead = ahead + take(tail, blocks - 1, 1)
        behind = part_in[par, 0]
        for k in range(1, sectors):
            behind = behind + part_in[par, k]
        far = below_in[par, 0]
        for k in range(1, sectors):
            far = far + below_in[par, k]
        behind = jnp.where(row_block == 0, far, pltpu.roll(behind, 2, 0))
        c = term[...]
        image = live_ref[...] * (
            energy_rows[...] * c + strength * (ahead + behind) - kinetic_scale * surf
        )
        even = lax.rem(lax.broadcasted_iota(jnp.int32, (rows, 1), 0), 2) == 0
        value = factor * jnp.where(
            even, pltpu.roll(image, rows - 1, 0), -pltpu.roll(image, 1, 0)
        )
        acc = total_inner[...] + value
        total_inner[...] = acc
        term[...] = jnp.where(last, acc, value)

        for copy in a_copies(par) + [b_copy(par, s) for s in range(1, sectors)]:
            copy.wait_send()

        @pl.when(has_below)
        def _():
            for copy in z_copies(par):
                copy.wait_send()

        @pl.when(has_above)
        def _():
            for s in range(sectors):
                y_copy(par, s).wait_send()

        surf_sends(st, lambda copy: copy.wait_send())
        point_sends(st, lambda copy: copy.wait_send())
        edge_sends(st, lambda copy: copy.wait_send())

        @pl.when(t < count - 1)
        def _():
            send_state(t + 1)
            send_back(t + 1)

        return carry

    lax.fori_loop(0, count, apply, 0)
    edge_wait((count - 1) % SLOTS, 0)
    edge_waits_beyond((count - 1) % SLOTS)
    correct_own(jnp.int32(count - 1), 0, False)
    final = total_inner[...]
    for p in range(2):
        inner_out[p] = jnp.concatenate(
            [final[2 * l + p : 2 * l + p + 1] for l in range(blocks)], axis=0
        )


def publish(inner_ref, outer_ref, inner_out, outer_out, sem):
    copies = [
        pltpu.make_async_copy(inner_ref, inner_out, sem.at[0]),
        pltpu.make_async_copy(outer_ref, outer_out, sem.at[1]),
    ]
    for copy in copies:
        copy.start()
    for copy in copies:
        copy.wait()


def local(
    planes,
    sectors,
    inner_state,
    outer_state,
    energies,
    dipole,
    surface,
    thresholds,
    coupling_coef,
    coupling_pattern,
    block_sizes,
    field_strength,
):
    blocks, rc, total = dipole.shape
    ch = coupling_coef.shape[1]
    nc, nr = outer_state.shape[1:]
    rows = 2 * blocks
    ext = -(-(nc + 2 * ch) // 128) * 128
    vmem = pl.BlockSpec(memory_space=pltpu.VMEM)
    hbm = pl.BlockSpec(memory_space=pltpu.HBM)
    dma = pltpu.SemaphoreType.DMA
    side = -(-ch // 128) * 128
    inner, outer = pl.pallas_call(
        functools.partial(kernel, planes, sectors, ch),
        out_shape=(
            jax.ShapeDtypeStruct((2, blocks, rc), f32),
            jax.ShapeDtypeStruct((2, nc, nr), f32),
        ),
        in_specs=[hbm] * 10,
        out_specs=(vmem, vmem),
        scratch_shapes=[
            pltpu.VMEM((2, blocks, rc), f32),
            pltpu.VMEM((blocks, rc), f32),
            pltpu.VMEM((nc, rc), f32),
            pltpu.VMEM((1, nc), f32),
            pltpu.VMEM((blocks, ch, ch), f32),
            pltpu.VMEM((blocks, ch, ch), jnp.int32),
            pltpu.VMEM((1, blocks), jnp.int32),
            pltpu.VMEM((1, STEPS), f32),
            dma((8,)),
            pltpu.VMEM((blocks * rc, total), f32),
            pltpu.VMEM((2 * blocks * rc, total), bf16),
            pltpu.VMEM((2 * blocks * total, rc), bf16),
            pltpu.VMEM((2 * ext, rc), bf16),
            pltpu.VMEM((2 * rc, ext), bf16),
            pltpu.VMEM((2 * nc, nc + 2 * ch), bf16),
            pltpu.VMEM((2, 2, nc + 2 * ch, nr), f32),
            pltpu.VMEM((2, 2, ch, nr), f32),
            pltpu.VMEM((rows, rc), f32),
            pltpu.VMEM((2, sectors, rows, rc), f32),
            pltpu.VMEM((2, rows, rc), f32),
            pltpu.VMEM((2, sectors, rows, rc), f32),
            pltpu.VMEM((sectors, rows, rc), f32),
            pltpu.VMEM((2, sectors, rows, rc), f32),
            pltpu.VMEM((sectors, rows, rc), f32),
            pltpu.VMEM((2, sectors, rows, rc), f32),
            pltpu.VMEM((blocks + 1, side, side), f32),
            pltpu.VMEM((rows, rc), f32),
            pltpu.VMEM((rows, rc), f32),
            pltpu.VMEM((rows, rc), f32),
            pltpu.VMEM((nc, 1), f32),
            pltpu.VMEM((2, 8, ext), f32),
            pltpu.VMEM((2 * SLOTS, 8, ext), f32),
            pltpu.VMEM((SLOTS, 3, 8, ext), f32),
            pltpu.VMEM((SLOTS, 3, 8, ext), f32),
            pltpu.VMEM((SLOTS, 3, sectors, 8, ext), f32),
            pltpu.VMEM((SLOTS, 8, ext), f32),
            dma((blocks,)), dma((8,)), dma(()), dma(()),
            dma((sectors,)), dma((2, sectors)),
            dma((sectors,)), dma((2, sectors)),
            dma((sectors,)), dma((2, sectors)),
            dma((sectors,)), dma((2, sectors)),
            dma((2,)), dma((2, 2)), dma((2,)), dma((2, 2)),
            dma((2, 3)), dma((SLOTS, 3)), dma((SLOTS, 3)),
            dma((3,)), dma((SLOTS, 3)),
            dma((sectors,)), dma((SLOTS,)),
        ],
        compiler_params=pltpu.CompilerParams(
            collective_id=0, has_side_effects=True, vmem_limit_bytes=56 * 1024 * 1024
        ),
    )(
        inner_state,
        outer_state,
        energies,
        dipole.reshape(blocks * rc, total),
        surface.reshape(nc, rc),
        thresholds.reshape(1, nc),
        coupling_coef,
        coupling_pattern,
        block_sizes.reshape(1, blocks),
        field_strength.reshape(1, STEPS),
    )
    return pl.pallas_call(
        publish,
        out_shape=(
            jax.ShapeDtypeStruct((2, blocks, rc), f32),
            jax.ShapeDtypeStruct((2, nc, nr), f32),
        ),
        in_specs=[vmem] * 2,
        out_specs=(hbm, hbm),
        scratch_shapes=[dma((2,))],
    )(inner, outer)


def solution(mesh):
    placed = (
        P(None, "inner", "outer"),
        P(None, "inner", "outer"),
        P("inner", "outer"),
        P("inner", "outer", None),
        P("inner", None, "outer"),
        P("inner"),
        P("inner", None, None),
        P("inner", None, None),
        P("inner"),
        P(),
    )
    return jax.shard_map(
        functools.partial(local, mesh.shape["inner"], mesh.shape["outer"]),
        mesh=mesh,
        in_specs=placed,
        out_specs=(P(None, "inner", "outer"), P(None, "inner", "outer")),
        check_vma=False,
    )
```

```python
import functools

import jax
import jax.numpy as jnp
from jax import lax
from jax.experimental import pallas as pl
from jax.experimental.pallas import tpu as pltpu
from jax.sharding import PartitionSpec as P

STEPS = 2
ORDER = 4

kinetic_scale = 3.125
time_step = 0.1

MESH = pl.DeviceIdType.MESH
f32 = jnp.float32
bf16 = jnp.bfloat16
NN = (((1,), (0,)), ((), ()))
SLOTS = 4


def halves(x):
    high = x.astype(bf16).astype(f32)
    return high, x - high


def split(x):
    high = x.astype(bf16)
    return high, (x - high.astype(f32)).astype(bf16)


def dot(a, b):
    return lax.dot_general(a, b, NN, preferred_element_type=f32)


def kernel(
    planes,
    sectors,
    ch,
    inner_hbm,
    outer_hbm,
    energy_hbm,
    dipole_hbm,
    surface_hbm,
    threshold_hbm,
    coef_hbm,
    pattern_hbm,
    size_hbm,
    field_hbm,
    inner_out,
    outer_out,
    inner_ref,
    energy_ref,
    surface_ref,
    threshold_ref,
    coef_ref,
    pattern_ref,
    size_ref,
    field_ref,
    sem_small,
    dip_full,
    dip_cat,
    dip_turn,
    surf_cat,
    surf_turn,
    mix_split,
    grid,
    halo_out,
    term,
    peer_in,
    first_out,
    above_in,
    part_out,
    part_in,
    far_out,
    below_in,
    pairs,
    live_ref,
    energy_rows,
    total_inner,
    diag_ref,
    raw_rows,
    edge_out,
    left_in,
    right_in,
    surf_in,
    point_in,
    sem_load,
    sem_outer,
    sem_g_send,
    sem_g_recv,
    sem_a_send,
    sem_a_recv,
    sem_z_send,
    sem_z_recv,
    sem_b_send,
    sem_b_recv,
    sem_y_send,
    sem_y_recv,
    sem_up_send,
    sem_up_recv,
    sem_down_send,
    sem_down_recv,
    sem_e_send,
    sem_left,
    sem_right,
    sem_surf_send,
    sem_surf,
    sem_point_send,
    sem_point,
):
    z = lax.axis_index("inner")
    me = lax.axis_index("outer")
    blocks, rc = energy_hbm.shape
    rows = 2 * blocks
    nc, nr = grid.shape[2] - 2 * ch, grid.shape[3]
    ext = edge_out.shape[2]
    depth = 2 * blocks * rc
    near = rows - 2
    has_below = z > 0
    has_above = z < planes - 1
    power = sectors & (sectors - 1) == 0

    def partner(s):
        if not power:
            return lax.rem(me + s, sectors)
        to, bit = me, 1
        while bit < sectors:
            if s & bit:
                to = to + bit * (1 - 2 * ((me // bit) % 2))
            bit *= 2
        return to

    def source(s):
        return partner(s) if power else lax.rem(me + sectors - s, sectors)

    def remote(src, dst, send, recv, plane, sector):
        return pltpu.make_async_remote_copy(
            src_ref=src,
            dst_ref=dst,
            send_sem=send,
            recv_sem=recv,
            device_id={"inner": plane, "outer": sector},
            device_id_type=MESH,
        )

    def wait(ref, sem):
        pltpu.make_async_copy(ref, ref, sem).wait()

    barrier = pltpu.get_barrier_semaphore()

    def greet(plane, s):
        pl.semaphore_signal(
            barrier,
            inc=1,
            device_id={"inner": plane, "outer": partner(s)},
            device_id_type=MESH,
        )

    for s in range(sectors - 1, 0, -1):
        greet(z, s)

    @pl.when(has_below)
    def _():
        for s in range(sectors - 1, -1, -1):
            greet(z - 1, s)

    @pl.when(has_above)
    def _():
        for s in range(sectors - 1, -1, -1):
            greet(z + 1, s)

    own = pl.ds(ch, nc)
    small_loads = [
        pltpu.make_async_copy(src, dst, sem_small.at[i])
        for i, (src, dst) in enumerate(
            (
                (inner_hbm, inner_ref),
                (size_hbm, size_ref),
                (coef_hbm, coef_ref),
                (pattern_hbm, pattern_ref),
                (surface_hbm, surface_ref),
                (threshold_hbm, threshold_ref),
                (energy_hbm, energy_ref),
                (field_hbm, field_ref),
            )
        )
    ]
    for load in small_loads:
        load.start()
    states = []
    for p in range(2):
        states.append(
            pltpu.make_async_copy(outer_hbm.at[p], grid.at[0, p, own, :], sem_outer.at[p])
        )
        states.append(
            pltpu.make_async_copy(
                outer_hbm.at[p, pl.ds(nc - ch, ch)], halo_out.at[p, 0], sem_outer.at[2 + p]
            )
        )
        states.append(
            pltpu.make_async_copy(
                outer_hbm.at[p, pl.ds(0, ch)], halo_out.at[p, 1], sem_outer.at[4 + p]
            )
        )
        states.append(
            pltpu.make_async_copy(outer_hbm.at[p], outer_out.at[p], sem_outer.at[6 + p])
        )
    for p in (1, 0):
        states[4 * p + 1].start()
        states[4 * p + 2].start()
    loads = [
        pltpu.make_async_copy(
            dipole_hbm.at[pl.ds(l * rc, rc)], dip_full.at[pl.ds(l * rc, rc)], sem_load.at[l]
        )
        for l in range(blocks)
    ]
    for load in loads:
        load.start()
    for p in range(2):
        states[4 * p].start()
        states[4 * p + 3].start()

    raw_rows[...] = jnp.zeros_like(raw_rows)

    @pl.when(z == 0)
    def _():
        below_in[...] = jnp.zeros_like(below_in)
        grid[:, :, 0:ch, :] = jnp.zeros((2, 2, ch, nr), f32)

    @pl.when(z == planes - 1)
    def _():
        above_in[...] = jnp.zeros_like(above_in)
        grid[:, :, ch + nc : 2 * ch + nc, :] = jnp.zeros((2, 2, ch, nr), f32)

    def channel_copies(slot, p):
        up = remote(
            halo_out.at[p, 0],
            grid.at[slot, p, pl.ds(0, ch), :],
            sem_up_send.at[p],
            sem_up_recv.at[slot, p],
            z + 1,
            me,
        )
        down = remote(
            halo_out.at[p, 1],
            grid.at[slot, p, pl.ds(ch + nc, ch), :],
            sem_down_send.at[p],
            sem_down_recv.at[slot, p],
            z - 1,
            me,
        )
        return up, down

    for load in small_loads:
        load.wait()

    side = pairs.shape[1]
    for l in range(blocks + 1):
        pairs[l, ch:side, :] = jnp.zeros((side - ch, side), f32)
    for l in range(blocks):
        pairs[l + 1, 0:ch, :] = jnp.zeros((ch, side), f32)
        pairs[l + 1, 0:ch, 0:ch] = coef_ref[l] * pattern_ref[l].astype(f32)

    @pl.when(z == 0)
    def _():
        pairs[0, 0:ch, :] = jnp.zeros((ch, side), f32)

    share = remote(
        pairs.at[blocks, pl.ds(0, ch), :],
        pairs.at[0, pl.ds(0, ch), :],
        sem_g_send,
        sem_g_recv,
        z + 1,
        me,
    )

    order_of = [(l, p) for l in range(blocks) for p in range(2)]
    position = me * rc + lax.broadcasted_iota(jnp.int32, (1, rc), 1)
    live_ref[...] = jnp.concatenate(
        [jnp.where(position < size_ref[:, l : l + 1], 1.0, 0.0) for l, p in order_of], axis=0
    )
    energy_rows[...] = jnp.concatenate([energy_ref[l : l + 1, :] for l, p in order_of], axis=0)
    term[...] = live_ref[...] * jnp.concatenate(
        [inner_ref[p, l : l + 1, :] for l, p in order_of], axis=0
    )
    total_inner[...] = term[...]

    small = lax.broadcasted_iota(jnp.int32, (nc, nc), 0) == lax.broadcasted_iota(
        jnp.int32, (nc, nc), 1
    )
    diag_ref[...] = 2.0 * kinetic_scale + jnp.sum(
        jnp.where(small, threshold_ref[...], 0.0), axis=1, keepdims=True
    )

    surface_ext = jnp.concatenate(
        [
            jnp.zeros((ch, rc), f32),
            surface_ref[...],
            jnp.zeros((ext - ch - nc, rc), f32),
        ],
        axis=0,
    )
    sh, sl = split(surface_ext)
    surf_cat[0:ext, :] = sh
    surf_cat[ext : 2 * ext, :] = sl
    surf_turn[0:rc, :] = sh.T
    surf_turn[rc : 2 * rc, :] = sl.T

    waits = (sectors - 1) + sectors * (
        jnp.where(has_below, 1, 0) + jnp.where(has_above, 1, 0)
    )
    pl.semaphore_wait(barrier, waits)

    @pl.when(has_above)
    def _():
        share.start()

    for p in (1, 0):
        states[4 * p + 1].wait()
        states[4 * p + 2].wait()
        up, down = channel_copies(0, p)

        @pl.when(has_above)
        def _():
            up.start()

        @pl.when(has_below)
        def _():
            down.start()

    count = STEPS * ORDER
    row_block = lax.broadcasted_iota(jnp.int32, (rows, 1), 0) // 2
    low_lane = ch + ch * (lax.broadcasted_iota(jnp.int32, (rows, ext), 0) // 2)
    lane_of = lax.broadcasted_iota(jnp.int32, (rows, ext), 1)
    own_lanes = (lane_of >= low_lane) & (lane_of < low_lane + ch)

    def eye(count, shift):
        return (
            lax.broadcasted_iota(jnp.int32, (count, ext), 0) + shift
            == lax.broadcasted_iota(jnp.int32, (count, ext), 1)
        )

    def to_row(col):
        return jnp.sum(jnp.where(eye(nc, ch), col, 0.0), axis=0, keepdims=True)

    def to_col(row, count, shift):
        return jnp.sum(jnp.where(eye(count, shift), row, 0.0), axis=1, keepdims=True)

    def spread(v, first, count):
        high, low = halves(v)
        zero = jnp.zeros_like(v)
        top, bottom = [], []
        for l in range(first, first + count):
            mine = row_block == l
            h = jnp.where(mine, high, 0.0)
            top += [h, h]
            bottom += [jnp.where(mine, low, 0.0), zero]
        return jnp.concatenate(
            [jnp.concatenate(top, axis=1), jnp.concatenate(bottom, axis=1)], axis=0
        ).astype(bf16)

    def stacked(v):
        high, low = halves(v)
        return jnp.concatenate(
            [
                jnp.concatenate([high, high], axis=1),
                jnp.concatenate([low, jnp.zeros_like(low)], axis=1),
            ],
            axis=0,
        ).astype(bf16)

    def fold(r):
        return r[:rows] + r[rows:]

    def edge_sends(st, f):
        def three(cond, src, dst, sem, send, sector):
            @pl.when(cond)
            def _():
                f(remote(src, dst(0), send.at[0], sem.at[st, 0], z, sector))

                @pl.when(has_below)
                def _():
                    f(remote(src, dst(2), send.at[1], sem.at[st, 2], z - 1, sector))

                @pl.when(has_above)
                def _():
                    f(remote(src, dst(1), send.at[2], sem.at[st, 1], z + 1, sector))

        three(
            me > 0,
            edge_out.at[st, pl.ds(0, 2)],
            lambda o: right_in.at[st, o, pl.ds(0, 2)],
            sem_right,
            sem_e_send.at[0],
            me - 1,
        )
        three(
            me < sectors - 1,
            edge_out.at[st + SLOTS, pl.ds(0, 2)],
            lambda o: left_in.at[st, o, pl.ds(0, 2)],
            sem_left,
            sem_e_send.at[1],
            me + 1,
        )

    def surf_sends(st, f):
        src = surf_in.at[st, 0, me, pl.ds(0, 2)]

        @pl.when(me > 0)
        def _():
            f(remote(src, src, sem_surf_send.at[0], sem_surf.at[st, 0], z, 0))

        @pl.when(has_below)
        def _():
            dst = surf_in.at[st, 2, me, pl.ds(0, 2)]
            f(remote(src, dst, sem_surf_send.at[1], sem_surf.at[st, 2], z - 1, 0))

        @pl.when(has_above)
        def _():
            dst = surf_in.at[st, 1, me, pl.ds(0, 2)]
            f(remote(src, dst, sem_surf_send.at[2], sem_surf.at[st, 1], z + 1, 0))

    def point_sends(st, f):
        @pl.when(me == 0)
        def _():
            src = point_in.at[st, pl.ds(0, 2)]
            for k in range(1, sectors):
                f(remote(src, src, sem_point_send.at[k], sem_point.at[st], z, k))

    def edge_wait(sl, o):
        @pl.when(me > 0)
        def _():
            wait(left_in.at[sl, o, pl.ds(0, 2)], sem_left.at[sl, o])

        @pl.when(me < sectors - 1)
        def _():
            wait(right_in.at[sl, o, pl.ds(0, 2)], sem_right.at[sl, o])

        @pl.when(me == 0)
        def _():
            first = 1 if o == 0 else 0
            wait(
                surf_in.at[sl, o, pl.ds(first, sectors - first), pl.ds(0, 2)],
                sem_surf.at[sl, o],
            )

    def edge_waits_beyond(sl):
        @pl.when(has_below)
        def _():
            edge_wait(sl, 1)

        @pl.when(has_above)
        def _():
            edge_wait(sl, 2)

    def edge_rows(sl, o):
        total_b = surf_in[sl, o, 0]
        for k in range(1, sectors):
            total_b = total_b + surf_in[sl, o, k]
        left = jnp.where(me == 0, total_b, left_in[sl, o])
        right = jnp.where(me == sectors - 1, 0.0, right_in[sl, o])
        if o == 1:
            left, right = jnp.where(has_below, left, 0.0), jnp.where(has_below, right, 0.0)
        if o == 2:
            left, right = jnp.where(has_above, left, 0.0), jnp.where(has_above, right, 0.0)
        return left, right

    lane = lax.broadcasted_iota(jnp.int32, (1, 128), 1)

    def scales(t):
        order = lax.rem(t, ORDER)
        factor = time_step / (order + 1).astype(f32)
        return factor * kinetic_scale, -factor * kinetic_scale

    def correct_own(t, par, refresh):
        valid = t >= 0
        sl = lax.rem(t + SLOTS, SLOTS)
        t = jnp.maximum(t, 0)
        left, right = [jnp.where(valid, row, 0.0) for row in edge_rows(sl, 0)]
        for d, scale in ((1, scales(t)[0]), (0, scales(t)[1])):
            first = jnp.where(lane == 0, scale * to_col(left[1 - d : 2 - d], nc, ch), 0.0)
            last = jnp.where(lane == 127, scale * to_col(right[1 - d : 2 - d], nc, ch), 0.0)
            outer_out[d, :, 0:128] += first
            outer_out[d, :, nr - 128 : nr] += last
            if refresh:
                grid[par, d, own, 0:128] += first
                grid[par, d, own, nr - 128 : nr] += last

    def a_copies(par):
        here = peer_in.at[par, me, pl.ds(0, near)]
        return [
            remote(here, here, sem_a_send.at[s], sem_a_recv.at[par, s], z, partner(s))
            for s in range(sectors - 1, 0, -1)
        ]

    def z_copies(par):
        return [
            remote(
                first_out.at[par, pl.ds(0, 2)],
                above_in.at[par, me, pl.ds(0, 2)],
                sem_z_send.at[s],
                sem_z_recv.at[par, s],
                z - 1,
                partner(s),
            )
            for s in range(sectors - 1, -1, -1)
        ]

    def b_copy(par, s):
        return remote(
            part_out.at[s, pl.ds(0, near)],
            part_in.at[par, me, pl.ds(0, near)],
            sem_b_send.at[s],
            sem_b_recv.at[par, s],
            z,
            partner(s),
        )

    def y_copy(par, s):
        return remote(
            far_out.at[s, pl.ds(0, 2)],
            below_in.at[par, me, pl.ds(0, 2)],
            sem_y_send.at[s],
            sem_y_recv.at[par, s],
            z + 1,
            partner(s),
        )

    def send_state(t):
        par = lax.rem(t, 2)
        c = term[...]
        first_out[par] = c
        peer_in[par, me] = pltpu.roll(c, rows - 2, 0)

        @pl.when(has_below)
        def _():
            for copy in z_copies(par):
                copy.start()

        for copy in a_copies(par):
            copy.start()

    row_of = lax.broadcasted_iota(jnp.int32, (8, 1), 0)

    def send_edges(t):
        st = lax.rem(t, SLOTS)
        edge_out[st] = raw_rows[0]
        edge_out[st + SLOTS] = raw_rows[1]

        @pl.when(t > 0)
        def _():
            sl = lax.rem(t + SLOTS - 1, SLOTS)
            edge_wait(sl, 0)
            one, zero = scales(t - 1)
            scale = jnp.where(row_of == 0, zero, one)
            for e, row in enumerate(edge_rows(sl, 0)):
                row = jnp.where(row_of == 0, pltpu.roll(row, 7, 0), pltpu.roll(row, 1, 0))
                edge_out[st + e * SLOTS] += scale * row

        @pl.when(me == 0)
        def _():
            point_in[st] = edge_out[st]

        point_sends(st, lambda copy: copy.start())
        edge_sends(st, lambda copy: copy.start())

    def send_back(t):
        par = lax.rem(t, 2)
        st = lax.rem(t, SLOTS)
        c = term[...]
        lhs = stacked(c)

        def product(l, s):
            at = pl.ds(pl.multiple_of(partner(s) * rc, 128), rc)
            return fold(dot(lhs, dip_cat[2 * l * rc : 2 * (l + 1) * rc, at]))

        def group(chosen):
            for s in chosen:
                far_out[s] = pltpu.roll(product(blocks - 1, s), 2, 0)
                back = jnp.zeros((rows, rc), f32)
                for l in range(blocks - 1):
                    back = jnp.where(row_block == l, product(l, s), back)
                if s:
                    part_out[s] = back
                else:
                    part_in[par, me] = back

            @pl.when(has_above)
            def _():
                for s in chosen:
                    y_copy(par, s).start()

            for s in chosen:
                if s:
                    b_copy(par, s).start()

        def send_surf():
            b = fold(dot(lhs, surf_turn[...]))
            b = jnp.where(own_lanes, b, 0.0)
            total_b = b
            for l in range(1, blocks):
                total_b = total_b + pltpu.roll(b, 2 * l, 0)
            surf_in[st, 0, me] = total_b
            surf_sends(st, lambda copy: copy.start())

        order = list(range(sectors - 1, -1, -1))
        group(order[: sectors // 2])
        send_surf()
        send_edges(t)
        group(order[sectors // 2 :])

    send_state(jnp.int32(0))
    for l in range(blocks):
        loads[l].wait()

        def divide(k, carry):
            at = pl.ds(pl.multiple_of(k * rc, 128), rc)
            high, low = split(dip_full[l * rc : (l + 1) * rc, at])
            dip_cat[2 * l * rc : (2 * l + 1) * rc, at] = high
            dip_cat[(2 * l + 1) * rc : (2 * l + 2) * rc, at] = low
            return carry

        lax.fori_loop(0, sectors, divide, 0, unroll=2)

    for p in range(2):
        states[4 * p].wait()
        states[4 * p + 3].wait()
        raw_rows[0, p : p + 1, :] = to_row(grid[0, p, own, 0:1])
        raw_rows[1, p : p + 1, :] = to_row(grid[0, p, own, nr - 1 : nr])
    send_back(jnp.int32(0))
    for l in range(blocks):

        def turn(k, carry):
            at = pl.ds(pl.multiple_of(k * rc, 128), rc)
            base = k * depth + 2 * l * rc
            high = dip_cat[2 * l * rc : (2 * l + 1) * rc, at]
            low = dip_cat[(2 * l + 1) * rc : (2 * l + 2) * rc, at]
            dip_turn[pl.ds(pl.multiple_of(base, 128), rc), :] = high.T
            dip_turn[pl.ds(pl.multiple_of(base + rc, 128), rc), :] = low.T
            return carry

        lax.fori_loop(0, sectors, turn, 0, unroll=4)

    @pl.when(has_below)
    def _():
        share.wait_recv()

    @pl.when(has_above)
    def _():
        share.wait_send()

    reach = -(-(nc + 2 * ch) // 128) * 128
    fill = jnp.zeros((ch, reach - side), f32)
    mixed_rows = []
    for l in range(blocks):
        upward = jnp.concatenate([pairs[l + 1, 0:ch, :], fill], axis=1)
        downward = jnp.concatenate([pairs[l].T[0:ch], fill], axis=1)
        upward = pltpu.roll(upward, (l + 2) * ch, 1)
        if l:
            downward = pltpu.roll(downward, l * ch, 1)
        mixed_rows.append((upward + downward)[:, 0 : nc + 2 * ch])
    mh, ml = split(jnp.concatenate(mixed_rows, axis=0))
    mix_split[0:nc, :] = mh
    mix_split[nc : 2 * nc, :] = ml

    def apply(t, carry):
        par = lax.rem(t, 2)
        nxt = 1 - par
        st = lax.rem(t, SLOTS)
        order = lax.rem(t, ORDER)
        step = lax.div(t, ORDER)
        strength = field_ref[:, 0:1]
        for i in range(1, STEPS):
            strength = jnp.where(step == i, field_ref[:, i : i + 1], strength)
        factor = time_step / (order + 1).astype(f32)
        last = order == ORDER - 1

        @pl.when(t > 0)
        def _():
            edge_waits_beyond(lax.rem(t + SLOTS - 1, SLOTS))

        def unit_wait(q):
            p = lax.rem(t + 1 + q, 2)
            up, down = channel_copies(par, p)
            up_old, down_old = channel_copies(par, 1 - p)

            @pl.when(has_below)
            def _():
                up.wait_recv()
                down_old.wait_send()

            @pl.when(has_above)
            def _():
                down.wait_recv()
                up_old.wait_send()

        def unit_start(q):
            p = lax.rem(t + 1 + q, 2)
            imag = p == 1
            past = jnp.maximum(t - 1, 0)
            sl = lax.rem(t + SLOTS - 1, SLOTS)
            one, zero = scales(past)
            scale = jnp.where(imag, one, zero)
            for o, start, shift in ((1, 0, nc), (2, ch + nc, ch)):
                left, right = [jnp.where(t > 0, row, 0.0) for row in edge_rows(sl, o)]
                left = jnp.where(imag, left[0:1], left[1:2])
                right = jnp.where(imag, right[0:1], right[1:2])
                at = pl.ds(start, ch)
                grid[par, p, at, 0:128] += jnp.where(
                    lane == 0, scale * to_col(left, ch, shift), 0.0
                )
                grid[par, p, at, nr - 128 : nr] += jnp.where(
                    lane == 127, scale * to_col(right, ch, shift), 0.0
                )
            gh, gl = split(grid[par, p])
            r = dot(mix_split[...], gh)
            return r[:nc] + r[nc:] + dot(mix_split[0:nc, :], gl)

        def unit_finish(q, coupled):
            p = lax.rem(t + 1 + q, 2)
            imag = p == 1
            x = grid[par, p, own, :]
            lanes = lax.broadcasted_iota(jnp.int32, (1, nr), 1)
            left = jnp.where(lanes == 0, 0.0, pltpu.roll(x, 1, 1))
            right = jnp.where(lanes == nr - 1, 0.0, pltpu.roll(x, nr - 1, 1))
            image = diag_ref[...] * x - kinetic_scale * (left + right) + strength * coupled
            value = jnp.where(imag, factor, -factor) * image
            acc = outer_out[1 - p] + value
            outer_out[1 - p] = acc
            value = jnp.where(last, acc, value)
            grid[nxt, 1 - p, own, :] = value
            raw_rows[0, pl.ds(1 - p, 1), :] = to_row(value[:, 0:1])
            raw_rows[1, pl.ds(1 - p, 1), :] = to_row(value[:, nr - 1 : nr])
            halo_out[1 - p, 0] = value[nc - ch : nc]
            halo_out[1 - p, 1] = value[0:ch]

        def unit_send(q):
            p = lax.rem(t + 1 + q, 2)
            up_new, down_new = channel_copies(nxt, 1 - p)

            @pl.when(jnp.logical_and(has_above, t < STEPS * ORDER - 1))
            def _():
                up_new.start()

            @pl.when(jnp.logical_and(has_below, t < STEPS * ORDER - 1))
            def _():
                down_new.start()

        def take_wait(group):
            for s in group:
                if s:
                    wait(peer_in.at[par, source(s), pl.ds(0, near)], sem_a_recv.at[par, s])

        def take(groups, first, count):
            total = jnp.zeros((rows, rc), f32)
            for group in (groups[0::2], groups[1::2]):
                sums = [None] * count
                for s in group:
                    k = source(s)
                    if first:
                        left = stacked(pltpu.roll(above_in[par, k], rows - 2, 0))
                    else:
                        left = stacked(peer_in[par, k])
                    for i in range(count):
                        base = k * depth + 2 * (first + i) * rc
                        at = pl.ds(pl.multiple_of(base, 128), 2 * rc)
                        part = dot(left, dip_turn[at, :])
                        sums[i] = part if sums[i] is None else sums[i] + part
                for i in range(count):
                    total = total + jnp.where(row_block == first + i, fold(sums[i]), 0.0)
            return total

        middle = list(range(2, sectors * 3 // 4))
        tail = list(range(sectors * 3 // 4, sectors))

        unit_wait(0)
        take_wait([0, 1])
        correct_own(t - 1, par, True)
        coupled = unit_start(0)
        ahead = take([0, 1], 0, blocks - 1)
        unit_finish(0, coupled)
        unit_send(0)

        unit_wait(1)
        take_wait(middle)
        coupled = unit_start(1)
        ahead = ahead + take(middle, 0, blocks - 1)
        unit_finish(1, coupled)
        unit_send(1)

        take_wait(tail)

        @pl.when(me > 0)
        def _():
            wait(point_in.at[st, pl.ds(0, 2)], sem_point.at[st])

        def far_wait(group):
            @pl.when(has_above)
            def _():
                for s in group:
                    wait(above_in.at[par, source(s), pl.ds(0, 2)], sem_z_recv.at[par, s])

        far_wait([0, 1] + middle)
        ahead = ahead + take(tail, 0, blocks - 1)
        point = jnp.concatenate([point_in[st, 0:2]] * blocks, axis=0)
        surf = fold(dot(stacked(jnp.where(own_lanes, point, 0.0)), surf_cat[...]))
        ahead = ahead + take([0, 1] + middle, blocks - 1, 1)

        for s in range(1, sectors):
            wait(part_in.at[par, source(s), pl.ds(0, near)], sem_b_recv.at[par, s])
        far_wait(tail)

        @pl.when(has_below)
        def _():
            for s in range(sectors):
                wait(below_in.at[par, source(s), pl.ds(0, 2)], sem_y_recv.at[par, s])

        ahead = ahead + take(tail, blocks - 1, 1)
        behind = part_in[par, 0]
        for k in range(1, sectors):
            behind = behind + part_in[par, k]
        far = below_in[par, 0]
        for k in range(1, sectors):
            far = far + below_in[par, k]
        behind = jnp.where(row_block == 0, far, pltpu.roll(behind, 2, 0))
        c = term[...]
        image = live_ref[...] * (
            energy_rows[...] * c + strength * (ahead + behind) - kinetic_scale * surf
        )
        even = lax.rem(lax.broadcasted_iota(jnp.int32, (rows, 1), 0), 2) == 0
        value = factor * jnp.where(
            even, pltpu.roll(image, rows - 1, 0), -pltpu.roll(image, 1, 0)
        )
        acc = total_inner[...] + value
        total_inner[...] = acc
        term[...] = jnp.where(last, acc, value)

        for copy in a_copies(par) + [b_copy(par, s) for s in range(1, sectors)]:
            copy.wait_send()

        @pl.when(has_below)
        def _():
            for copy in z_copies(par):
                copy.wait_send()

        @pl.when(has_above)
        def _():
            for s in range(sectors):
                y_copy(par, s).wait_send()

        surf_sends(st, lambda copy: copy.wait_send())
        point_sends(st, lambda copy: copy.wait_send())
        edge_sends(st, lambda copy: copy.wait_send())

        @pl.when(t < count - 1)
        def _():
            send_state(t + 1)
            send_back(t + 1)

        return carry

    lax.fori_loop(0, count, apply, 0)
    edge_wait((count - 1) % SLOTS, 0)
    edge_waits_beyond((count - 1) % SLOTS)
    correct_own(jnp.int32(count - 1), 0, False)
    final = total_inner[...]
    for p in range(2):
        inner_out[p] = jnp.concatenate(
            [final[2 * l + p : 2 * l + p + 1] for l in range(blocks)], axis=0
        )


def publish(inner_ref, outer_ref, inner_out, outer_out, inner_held, outer_held, sems):
    count = outer_held.shape[0] * 2
    nc = outer_held.shape[1] // 2
    pieces = [(inner_ref, inner_held, inner_out)]
    for i in range(count):
        at = (i // 2, pl.ds((i % 2) * nc, nc))
        pieces.append((outer_ref.at[at], outer_held.at[at], outer_out.at[at]))
    takes = [pltpu.make_async_copy(a, b, sems.at[0, i]) for i, (a, b, _) in enumerate(pieces)]
    gives = [pltpu.make_async_copy(b, c, sems.at[1, i]) for i, (_, b, c) in enumerate(pieces)]
    for take in takes:
        take.start()
    for take, give in zip(takes, gives):
        take.wait()
        give.start()
    for give in gives:
        give.wait()


def local(
    planes,
    sectors,
    inner_state,
    outer_state,
    energies,
    dipole,
    surface,
    thresholds,
    coupling_coef,
    coupling_pattern,
    block_sizes,
    field_strength,
):
    blocks, rc, total = dipole.shape
    ch = coupling_coef.shape[1]
    nc, nr = outer_state.shape[1:]
    rows = 2 * blocks
    ext = -(-(nc + 2 * ch) // 128) * 128
    vmem = pl.BlockSpec(memory_space=pltpu.VMEM)
    hbm = pl.BlockSpec(memory_space=pltpu.HBM)
    dma = pltpu.SemaphoreType.DMA
    side = -(-ch // 128) * 128
    inner, outer = pl.pallas_call(
        functools.partial(kernel, planes, sectors, ch),
        out_shape=(
            jax.ShapeDtypeStruct((2, blocks, rc), f32),
            jax.ShapeDtypeStruct((2, nc, nr), f32),
        ),
        in_specs=[hbm] * 10,
        out_specs=(vmem, vmem),
        scratch_shapes=[
            pltpu.VMEM((2, blocks, rc), f32),
            pltpu.VMEM((blocks, rc), f32),
            pltpu.VMEM((nc, rc), f32),
            pltpu.VMEM((1, nc), f32),
            pltpu.VMEM((blocks, ch, ch), f32),
            pltpu.VMEM((blocks, ch, ch), jnp.int32),
            pltpu.VMEM((1, blocks), jnp.int32),
            pltpu.VMEM((1, STEPS), f32),
            dma((8,)),
            pltpu.VMEM((blocks * rc, total), f32),
            pltpu.VMEM((2 * blocks * rc, total), bf16),
            pltpu.VMEM((2 * blocks * total, rc), bf16),
            pltpu.VMEM((2 * ext, rc), bf16),
            pltpu.VMEM((2 * rc, ext), bf16),
            pltpu.VMEM((2 * nc, nc + 2 * ch), bf16),
            pltpu.VMEM((2, 2, nc + 2 * ch, nr), f32),
            pltpu.VMEM((2, 2, ch, nr), f32),
            pltpu.VMEM((rows, rc), f32),
            pltpu.VMEM((2, sectors, rows, rc), f32),
            pltpu.VMEM((2, rows, rc), f32),
            pltpu.VMEM((2, sectors, rows, rc), f32),
            pltpu.VMEM((sectors, rows, rc), f32),
            pltpu.VMEM((2, sectors, rows, rc), f32),
            pltpu.VMEM((sectors, rows, rc), f32),
            pltpu.VMEM((2, sectors, rows, rc), f32),
            pltpu.VMEM((blocks + 1, side, side), f32),
            pltpu.VMEM((rows, rc), f32),
            pltpu.VMEM((rows, rc), f32),
            pltpu.VMEM((rows, rc), f32),
            pltpu.VMEM((nc, 1), f32),
            pltpu.VMEM((2, 8, ext), f32),
            pltpu.VMEM((2 * SLOTS, 8, ext), f32),
            pltpu.VMEM((SLOTS, 3, 8, ext), f32),
            pltpu.VMEM((SLOTS, 3, 8, ext), f32),
            pltpu.VMEM((SLOTS, 3, sectors, 8, ext), f32),
            pltpu.VMEM((SLOTS, 8, ext), f32),
            dma((blocks,)), dma((8,)), dma(()), dma(()),
            dma((sectors,)), dma((2, sectors)),
            dma((sectors,)), dma((2, sectors)),
            dma((sectors,)), dma((2, sectors)),
            dma((sectors,)), dma((2, sectors)),
            dma((2,)), dma((2, 2)), dma((2,)), dma((2, 2)),
            dma((2, 3)), dma((SLOTS, 3)), dma((SLOTS, 3)),
            dma((3,)), dma((SLOTS, 3)),
            dma((sectors,)), dma((SLOTS,)),
        ],
        compiler_params=pltpu.CompilerParams(
            collective_id=0, has_side_effects=True, vmem_limit_bytes=56 * 1024 * 1024
        ),
    )(
        inner_state,
        outer_state,
        energies,
        dipole.reshape(blocks * rc, total),
        surface.reshape(nc, rc),
        thresholds.reshape(1, nc),
        coupling_coef,
        coupling_pattern,
        block_sizes.reshape(1, blocks),
        field_strength.reshape(1, STEPS),
    )
    return pl.pallas_call(
        publish,
        out_shape=(
            jax.ShapeDtypeStruct((2, blocks, rc), f32),
            jax.ShapeDtypeStruct((2, nc, nr), f32),
        ),
        in_specs=[hbm] * 2,
        out_specs=(hbm, hbm),
        scratch_shapes=[
            pltpu.VMEM((2, blocks, rc), f32),
            pltpu.VMEM((2, nc, nr), f32),
            dma((2, 5)),
        ],
    )(inner, outer)


def solution(mesh):
    placed = (
        P(None, "inner", "outer"),
        P(None, "inner", "outer"),
        P("inner", "outer"),
        P("inner", "outer", None),
        P("inner", None, "outer"),
        P("inner"),
        P("inner", None, None),
        P("inner", None, None),
        P("inner"),
        P(),
    )
    return jax.shard_map(
        functools.partial(local, mesh.shape["inner"], mesh.shape["outer"]),
        mesh=mesh,
        in_specs=placed,
        out_specs=(P(None, "inner", "outer"), P(None, "inner", "outer")),
        check_vma=False,
    )
```
